32 devices in a mesh: elem: 8 (over z, y), bucket: 4 (over x, core).
Axes of the slice: x: 2, y: 2, z: 4, core: 2. Of those that a mesh axis runs over, the one named last changes fastest.
Arguments:
- node_data: float32 [24, 98304], P(None, 'elem'), may hold values from -6 to 6
- eroded: int32 [4096], P('elem'), may hold values from 0 to 2047, as said below
- bucket_map: int32 [98304], P('elem'), may hold values from 0 to 63, as said below
- seg_point: float32 [64, 3, 512], P('elem', None, 'bucket'), may hold values from -3 to 3
- seg_angle: float32 [64, 2, 512], P('elem', None, 'bucket'), may hold values from -3.140625 to 3.140625
Outputs:
- face_force: float32 [3, 24576], P(None, 'elem')
The draws below stay inside these ranges and needn't reach their ends.
Inputs may be any that keep to these rules, and one draw needn't show every extreme that they name: `eroded`: the 512 entries of one index of elem are distinct local element numbers. `bucket_map`: among the faces of the elements listed in eroded, those of one index of elem name one bucket at most 80 times; in every draw some bucket is named exactly 80 times by every index of elem.
All inputs are finite; a program needn't handle non-finite values.
Results may differ from the reference program's by a relative error of at most 0.00012.
Values sent between devices are 32-bit elements; how exact they have to be, the bound alone decides.
A program may use at most 64 MiB of HBM per device.

```python
import jax
import jax.numpy as jnp
from jax import lax

ELEM_DEV = 2048
ERODE_DEV = 512
SLOT = 80
BUCKETS = 64
SEGS = 512
FACES = 98304
UNCOVERED = 24576
N_ELEM = 8


def erosion_plan(key):
    plan_key = jax.random.fold_in(key, 11)
    elem_key, pool_key, hot_key, fill_key = jax.random.split(plan_key, 4)
    elem_iota = jnp.arange(ELEM_DEV, dtype=jnp.int32)
    elem_scores = jax.random.randint(elem_key, (N_ELEM, ELEM_DEV), 0, 65536, dtype=jnp.int32) * ELEM_DEV + elem_iota[None, :]
    eroded = jnp.argsort(elem_scores, axis=1)[:, :ERODE_DEV].astype(jnp.int32)
    pool_size = BUCKETS * SLOT
    pool_iota = jnp.arange(pool_size, dtype=jnp.int32)
    pool_ids = pool_iota // SLOT
    hot_bucket = jax.random.randint(hot_key, (), 0, BUCKETS, dtype=jnp.int32)
    scores = jax.random.randint(pool_key, (N_ELEM, pool_size), 0, 65536, dtype=jnp.int32) * pool_size + pool_iota[None, :]
    scores = jnp.where((pool_ids == hot_bucket)[None, :], pool_iota[None, :] - pool_size, scores)
    pool_order = jnp.argsort(scores, axis=1)[:, :6 * ERODE_DEV]
    chosen = pool_ids[pool_order].astype(jnp.int32)
    background = jax.random.randint(fill_key, (N_ELEM, 6 * ELEM_DEV), 0, BUCKETS, dtype=jnp.int32)
    sides = jnp.arange(6, dtype=jnp.int32)
    face_index = (6 * eroded[:, :, None] + sides[None, None, :]).reshape(N_ELEM, 6 * ERODE_DEV)
    device_rows = jnp.broadcast_to(jnp.arange(N_ELEM, dtype=jnp.int32)[:, None], face_index.shape)
    bucket_map = background.at[device_rows, face_index].set(chosen)
    return (eroded.reshape(-1), bucket_map.reshape(-1))


def draw_eroded(key, part):
    return erosion_plan(key)[0]


def draw_bucket_map(key, part):
    return erosion_plan(key)[1]


def level_of(stream_key, dims, cuts, least, top_value):
    level = 1.0
    for axis_at, shards_of in cuts:
        heights = jax.random.uniform(jax.random.fold_in(jax.random.fold_in(stream_key, 6), axis_at), (shards_of,), jnp.float32, least / len(cuts), top_value / len(cuts))
        level = level * jnp.repeat(jnp.exp(heights), dims[axis_at] // shards_of).reshape((-1,) + (1,) * (len(dims) - 1 - axis_at))
    return level


def normal_values(own_key, shape, deviation, most, shards=(), held_as=jnp.bfloat16):
    factor_of = level_of(own_key, shape, shards, -0.22, 0.18) if shards else 1.0
    entries = jax.random.normal(own_key, shape, jnp.float32) * deviation * factor_of
    return jnp.minimum(jnp.maximum(entries, -most), most).astype(held_as)


def setup_inputs(seed: int = 0) -> dict:
    key_list = jax.random.split(jax.random.key(seed), 6)
    node_data = normal_values(key_list[0], (24, FACES), 1.0, 6.0, ((1, 8),), jnp.float32)
    eroded = draw_eroded(jax.random.fold_in(key_list[5], 71), 0)
    bucket_map = draw_bucket_map(jax.random.fold_in(key_list[5], 71), 0)
    seg_point = normal_values(key_list[3], (BUCKETS, 3, SEGS), 0.5, 3.0, ((0, 8), (2, 4)), jnp.float32)
    seg_angle = jnp.clip(jax.random.uniform(key_list[4], (BUCKETS, 2, SEGS), jnp.float32, -3.140625, 3.140625), -3.140625, 3.140625)
    return dict(node_data=node_data, eroded=eroded, bucket_map=bucket_map, seg_point=seg_point, seg_angle=seg_angle)


STIFFNESS = 20.0
DAMPING = 0.5

def face_geometry(payload):
    corner = payload[0:12].reshape(4, 3, -1)
    motion = payload[12:24].reshape(4, 3, -1)
    centroid = 0.25 * (corner[0] + corner[1] + corner[2] + corner[3])
    first_edge = corner[2] - corner[0]
    second_edge = corner[3] - corner[1]
    area_x = 0.5 * (first_edge[1] * second_edge[2] - first_edge[2] * second_edge[1])
    area_y = 0.5 * (first_edge[2] * second_edge[0] - first_edge[0] * second_edge[2])
    area_z = 0.5 * (first_edge[0] * second_edge[1] - first_edge[1] * second_edge[0])
    velocity = 0.25 * (motion[0] + motion[1] + motion[2] + motion[3])
    return jnp.concatenate([centroid, jnp.stack([area_x, area_y, area_z]), velocity], axis=0)

def unit_normal(angles):
    return jnp.stack([jnp.cos(angles[:, 0]) * jnp.sin(angles[:, 1]), jnp.sin(angles[:, 0]) * jnp.sin(angles[:, 1]), jnp.cos(angles[:, 1])], axis=1)

def penalty_terms(geometry, point, normal, stiff):
    offset = geometry[0:3, :, None] - point
    dist_sq = offset[0] * offset[0] + offset[1] * offset[1] + offset[2] * offset[2]
    gap_value = offset[0] * normal[0] + offset[1] * normal[1] + offset[2] * normal[2]
    closing = geometry[6][:, None] * normal[0] + geometry[7][:, None] * normal[1] + geometry[8][:, None] * normal[2]
    projected = jnp.abs(geometry[3][:, None] * normal[0] + geometry[4][:, None] * normal[1] + geometry[5][:, None] * normal[2])
    depth_in = jnp.maximum(-gap_value, 0.0)
    weight = jnp.exp(-0.5 * dist_sq)
    return weight * depth_in * (stiff - DAMPING * closing) * projected

def reference(node_data, eroded, bucket_map, seg_point, seg_angle):
    local = eroded.reshape(N_ELEM, ERODE_DEV)
    sides = jnp.arange(6, dtype=jnp.int32)
    face_local = (6 * local[:, :, None] + sides[None, None, :]).reshape(N_ELEM, 6 * ERODE_DEV)
    offsets = (jnp.arange(N_ELEM, dtype=jnp.int32) * (6 * ELEM_DEV)).astype(jnp.int32)
    face_global = (face_local + offsets[:, None]).reshape(-1).astype(jnp.int32)
    bucket = bucket_map[face_global]
    geometry = face_geometry(node_data[:, face_global])
    counts = jnp.zeros((BUCKETS,), jnp.float32).at[bucket].add(1.0)
    stiffness = STIFFNESS * lax.rsqrt(jnp.maximum(counts, 1.0))
    normal_all = unit_normal(seg_angle)
    block_count = UNCOVERED // 128
    geo_blocks = geometry.reshape(9, block_count, 128).transpose(1, 0, 2)
    id_blocks = bucket.reshape(block_count, 128)

    def block_force(items):
        geo, block_ids = items
        point = seg_point[block_ids].transpose(1, 0, 2)
        normal = normal_all[block_ids].transpose(1, 0, 2)
        stiff = stiffness[block_ids][:, None]
        traction = penalty_terms(geo, point, normal, stiff)
        return lax.optimization_barrier(jnp.sum(traction[None, :, :] * normal, axis=2))
    forces = lax.map(block_force, (geo_blocks, id_blocks))
    return forces.transpose(1, 0, 2).reshape(3, UNCOVERED)
```

```python
import functools
import math

import jax
import jax.numpy as jnp
from jax import lax
from jax.experimental import pallas as pl
from jax.experimental.pallas import tpu as pltpu
from jax.sharding import PartitionSpec as P

STIFFNESS = 20.0
DAMPING = 0.5
SCALE = math.sqrt(0.5 / math.log(2.0))
LANES = 128
SIDES = 6
BLOCK = SIDES * LANES
F32 = jnp.float32
BF16 = jnp.bfloat16


def split3(x):
    hi = x.astype(BF16).astype(F32)
    rest = x - hi
    mid = rest.astype(BF16).astype(F32)
    return hi, mid, rest - mid


def sin_cos(x):
    k = jnp.floor(x * 0.6366197723675814 + 0.5)
    r = x - k * 1.5703125
    r = r - k * 4.837512969970703125e-4
    r = r - k * 7.54978995489188216e-8
    z = r * r
    s = ((-1.9515295891e-4 * z + 8.3321608736e-3) * z - 1.6666654611e-1) * z * r + r
    c = ((2.443315711809948e-5 * z - 1.388731625493765e-3) * z + 4.166664568298827e-2) * z * z
    c = c - 0.5 * z + 1.0
    q = k.astype(jnp.int32) & 3
    odd = (q & 1) == 1
    sin = jnp.where(odd, c, s)
    cos = jnp.where(odd, s, c)
    sin = jnp.where(q >= 2, -sin, sin)
    cos = jnp.where((q == 1) | (q == 2), -cos, cos)
    return sin, cos


def mm(a, b, contract=((1,), (0,))):
    return lax.dot_general(a, b, (contract, ((), ())), preferred_element_type=F32)


def partner(me, m, n):
    if n & (n - 1):
        return lax.rem(me + m, n)
    to, bit = 0, 1
    while bit < n:
        to = to + bit * lax.rem(me // bit + (m // bit) % 2, 2)
        bit *= 2
    return to


def source_of(me, m, n):
    return lax.rem(me + n - m, n) if n & (n - 1) else partner(me, m, n)


def blocks_of(n, f):
    if n == 1:
        f(0)
    else:
        pl.loop(0, n)(f)


def kernel(
    n_elem, n_buck, node_any, eroded_any, bmap_any, spoint_any, sangle_any, out,
    node, eroded, bmap, spoint, sangle,
    perm, pick, rows, faces, onehot, points, angles, values, seg_t, counts,
    sel0, sel1, parts,
    in_sem, seg_send, seg_recv, cnt_send, cnt_recv, par_send, par_recv,
):
    me = lax.axis_index("elem")
    mb = lax.axis_index("bucket")
    own, segs = sangle.shape[0], sangle.shape[2]
    buckets = own * n_elem
    count = eroded.shape[1]
    jblocks = count // LANES
    blocks = node.shape[1] // BLOCK
    nfaces = SIDES * count
    chunks, wide = parts.shape[1], parts.shape[3]
    mesh_ids = pl.DeviceIdType.MESH

    barrier = pltpu.get_barrier_semaphore()
    for m in range(n_elem - 1, 0, -1):
        to = {"elem": partner(me, m, n_elem)}
        pl.semaphore_signal(barrier, inc=1, device_id=to, device_id_type=mesh_ids)
    for d in range(1, n_buck):
        to = {"bucket": lax.rem(mb + d, n_buck)}
        pl.semaphore_signal(barrier, inc=1, device_id=to, device_id_type=mesh_ids)
    loads = [
        pltpu.make_async_copy(src, dst, in_sem.at[i])
        for i, (src, dst) in enumerate([
            (spoint_any, spoint), (sangle_any, sangle), (eroded_any, eroded),
            (bmap_any, bmap), (node_any, node),
        ])
    ]
    for load in loads:
        load.start()

    col = lax.broadcasted_iota(jnp.int32, (1, BLOCK), 1)
    source = SIDES * (col & (LANES - 1)) + (col // LANES)
    for i in range(BLOCK // 256):
        r = lax.broadcasted_iota(jnp.int32, (256, BLOCK), 0) + i * 256
        perm[i * 256:(i + 1) * 256, :] = jnp.where(r == source, 1.0, 0.0).astype(BF16)

    def seg_copies(m, owner, target):
        at = pl.ds(pl.multiple_of(owner * own, own), own)
        return [
            pltpu.make_async_remote_copy(
                src_ref=src, dst_ref=dst,
                send_sem=seg_send.at[i, m - 1], recv_sem=seg_recv.at[i, m - 1],
                device_id={"elem": target}, device_id_type=mesh_ids,
            )
            for i, (src, dst) in enumerate(
                [(spoint, points.at[:, at]), (sangle, angles.at[at])]
            )
        ]

    loads[0].wait()
    loads[1].wait()
    pl.semaphore_wait(barrier, n_elem + n_buck - 2)
    for m in range(n_elem - 1, 0, -1):
        for c in seg_copies(m, me, partner(me, m, n_elem)):
            c.start()

    loads[2].wait()
    loads[3].wait()
    erode = eroded[...]
    high = lax.broadcasted_iota(jnp.int32, (blocks, count), 0) == erode // LANES
    low = lax.broadcasted_iota(jnp.int32, (LANES, count), 0) == lax.rem(erode, LANES)
    mask = mm(
        jnp.where(high, 1.0, 0.0).astype(BF16), jnp.where(low, 1.0, 0.0).astype(BF16), ((1,), (1,))
    )
    first = SIDES * lax.broadcasted_iota(jnp.int32, (LANES, BLOCK), 0)
    away = lax.broadcasted_iota(jnp.int32, (LANES, BLOCK), 1) - first
    spread = jnp.where((away >= 0) & (away < SIDES), 1.0, 0.0).astype(BF16)
    mask = mm(mask.astype(BF16), spread)

    chunk = min(buckets, LANES)

    def count_block(b):
        iota = lax.broadcasted_iota(jnp.int32, (chunk, LANES), 0) + b * chunk
        total = jnp.zeros((chunk, LANES), F32)
        for r in range(blocks):
            ids = jnp.where(mask[r:r + 1] > 0.5, bmap[:, r * BLOCK:(r + 1) * BLOCK], -1)
            for g in range(SIDES):
                hit = iota == ids[:, g * LANES:(g + 1) * LANES]
                total = total + jnp.where(hit, 1.0, 0.0)
        if chunk < LANES:
            total = jnp.concatenate([total, jnp.zeros((LANES - chunk, LANES), F32)], axis=0)
        sums = mm(jnp.ones((8, LANES), BF16), total.astype(BF16), ((1,), (1,)))
        at = 0 if buckets <= LANES else pl.ds(pl.multiple_of(b * LANES, LANES), LANES)
        if buckets <= LANES:
            counts[me] = sums[0:1]
        else:
            counts[me, :, at] = sums[0:1]

    blocks_of(buckets // chunk, count_block)

    def cnt_copy(m, owner, target):
        return pltpu.make_async_remote_copy(
            src_ref=counts.at[owner], dst_ref=counts.at[owner],
            send_sem=cnt_send.at[m - 1], recv_sem=cnt_recv.at[m - 1],
            device_id={"elem": target}, device_id_type=mesh_ids,
        )

    for m in range(n_elem - 1, 0, -1):
        cnt_copy(m, me, partner(me, m, n_elem)).start()

    for i in range(pick.shape[0] // 256):
        r = lax.broadcasted_iota(jnp.int32, (256, count), 0) + i * 256
        pick[i * 256:(i + 1) * 256, :] = jnp.where(r == erode, 1.0, 0.0).astype(BF16)

    loads[4].wait()
    group = 4
    for g in range(blocks // group):
        stack = []
        for i in range(g * group, (g + 1) * group):
            lanes = slice(i * BLOCK, (i + 1) * BLOCK)
            c = [node[3 * v:3 * v + 3, lanes] for v in range(8)]
            e1, e2 = c[2] - c[0], c[3] - c[1]
            r1 = jnp.concatenate([e1[1:3], e1[0:1]], axis=0)
            r2 = jnp.concatenate([e2[1:3], e2[0:1]], axis=0)
            area = 0.5 * (e1 * r2 - r1 * e2)
            centroid = 0.25 * (((c[0] + c[1]) + c[2]) + c[3])
            velocity = 0.25 * (((c[4] + c[5]) + c[6]) + c[7])
            ids = bmap[:, lanes].astype(F32)
            two = jnp.zeros((2, BLOCK), F32)
            four = jnp.zeros((4, BLOCK), F32)
            first = jnp.concatenate([centroid, area, two], axis=0)
            second = jnp.concatenate([velocity, ids, four], axis=0)
            a, b = split3(first), split3(second)
            stack += [a[0], b[0], a[1], b[1], a[2]]
        apart = mm(jnp.concatenate(stack, axis=0).astype(BF16), perm[...]).astype(BF16)
        for i in range(group):
            at = (g * group + i) * LANES
            for s in range(SIDES):
                rows[s * 40:(s + 1) * 40, at:at + LANES] = apart[
                    i * 40:(i + 1) * 40, s * LANES:(s + 1) * LANES
                ]

    taken = mm(rows[...], pick[...]).astype(BF16)
    stack = []
    for j in range(jblocks):
        lanes = slice(j * LANES, (j + 1) * LANES)
        stack.append(
            jnp.concatenate([taken[s * 40:(s + 1) * 40, lanes] for s in range(SIDES)], axis=1)
        )
    mixed = mm(jnp.concatenate(stack, axis=0), perm[...], ((1,), (1,)))
    for j in range(jblocks):
        t = [mixed[j * 40 + i * 8:j * 40 + i * 8 + 8] for i in range(5)]
        lanes = slice(j * BLOCK, (j + 1) * BLOCK)
        faces[0:8, lanes] = (t[0] + t[2]) + t[4]
        faces[8:16, lanes] = t[1] + t[3]

    def hot_block(b):
        for j in range(nfaces // 512):
            lanes = slice(j * 512, (j + 1) * 512)
            iota = lax.broadcasted_iota(jnp.int32, (chunk, 512), 0) + b * chunk
            hit = iota == faces[11:12, lanes].astype(jnp.int32)
            onehot[pl.ds(b * chunk, chunk), lanes] = jnp.where(hit, 1.0, 0.0).astype(BF16)

    blocks_of(buckets // chunk, hot_block)

    def unfold(owner, p, a):
        at = pl.ds(pl.multiple_of(owner * own, own), own)
        sin0, cos0 = sin_cos(a[:, 0, :])
        sin1, cos1 = sin_cos(a[:, 1, :])
        x, y, z = [SCALE * p[i] for i in range(3)]
        for i, v in enumerate([x, y, z, cos0 * sin1, sin0 * sin1, cos1]):
            values[i, at, :] = v

    unfold(me, spoint[...], sangle[...])
    for m in range(1, n_elem):
        owner = source_of(me, m, n_elem)
        for cp in seg_copies(m, owner, me):
            cp.wait_recv()
        at = pl.ds(pl.multiple_of(owner * own, own), own)
        unfold(owner, points[:, at, :], angles[at])

    chunk = min(buckets, LANES // 2)

    def lay_out(b):
        for i in range(6):
            v = values[i, pl.ds(pl.multiple_of(b * chunk, chunk), chunk), :]
            stack = jnp.concatenate(list(split3(v)) + [jnp.zeros_like(v)], axis=0)
            lanes = pl.ds(pl.multiple_of(b * 4 * chunk, LANES), 4 * chunk)
            seg_t[i * segs:(i + 1) * segs, lanes] = stack.T.astype(BF16)

    blocks_of(buckets // chunk, lay_out)

    for m in range(1, n_elem):
        cnt_copy(m, source_of(me, m, n_elem), me).wait_recv()
    whole = counts[0]
    for i in range(1, n_elem):
        whole = whole + counts[i]
    stiff = (STIFFNESS / SCALE) * lax.rsqrt(jnp.maximum(whole[:, :buckets], 1.0))
    hi, mid, lo = split3(jnp.broadcast_to(stiff, (16, buckets)))
    pieces = []
    for b in range(0, buckets, chunk):
        cut = slice(b, b + chunk)
        pieces += [hi[:, cut], mid[:, cut], lo[:, cut], jnp.zeros((16, chunk), F32)]
    seg_t[6 * segs:6 * segs + 16, :] = jnp.concatenate(pieces, axis=1).astype(BF16)

    half = 256
    steps = nfaces // half

    def select(it, sel):
        hot = onehot[:, pl.ds(pl.multiple_of(it * half, half), half)]
        hot = [hot[b:b + chunk] for b in range(0, buckets, chunk) for _ in range(4)]
        sel[...] = mm(seg_t[...], jnp.concatenate(hot, axis=0))

    def forces(it, c, at, sel):
        for lt in range(half // LANES):
            g = faces[:, pl.ds(pl.multiple_of(it * half + lt * LANES, LANES), LANES)]
            cx, cy, cz, az, ax, ay, _, _, vx, vy, vz = [
                jnp.broadcast_to(g[i:i + 1], (8, LANES)) for i in range(11)
            ]
            cx, cy, cz = SCALE * cx, SCALE * cy, SCALE * cz
            damp = DAMPING / SCALE
            vx, vy, vz = damp * vx, damp * vy, damp * vz
            tile = slice(lt * LANES, (lt + 1) * LANES)
            stf = sel[6 * segs:6 * segs + 8, tile]
            acc = [jnp.zeros((8, LANES), F32) for _ in range(3)]
            for r in range(segs // 8):
                px, py, pz, nx, ny, nz = [
                    sel[q * segs + r * 8:q * segs + r * 8 + 8, tile] for q in range(6)
                ]
                ox, oy, oz = px - cx, py - cy, pz - cz
                dist = ox * ox + oy * oy + oz * oz
                depth = jnp.maximum(ox * nx + oy * ny + oz * nz, 0.0)
                proj = jnp.abs(ax * nx + ay * ny + az * nz)
                push = stf - (vx * nx + vy * ny + vz * nz)
                traction = (jnp.exp2(-dist) * depth) * (push * proj)
                for k, n in enumerate((nx, ny, nz)):
                    acc[k] = acc[k] + traction * n
            for k in range(3):
                total = jnp.sum(acc[k], axis=0, keepdims=True)
                parts[mb, c, k:k + 1, at + lt * LANES:at + (lt + 1) * LANES] = total

    def par_copy(c, d, owner, target):
        return pltpu.make_async_remote_copy(
            src_ref=parts.at[owner, c], dst_ref=parts.at[owner, c],
            send_sem=par_send.at[c, d - 1], recv_sem=par_recv.at[c, d - 1],
            device_id={"bucket": target}, device_id_type=mesh_ids,
        )

    select(0, sel0)

    def step(c, carry):
        it = 2 * c
        select(it + 1, sel1)
        forces(it, c, 0, sel0)
        select(lax.rem(it + 2, steps), sel0)
        forces(it + 1, c, half, sel1)
        for d in range(1, n_buck):
            par_copy(c, d, mb, lax.rem(mb + d, n_buck)).start()
        return carry

    lax.fori_loop(0, chunks, step, 0)

    for c in range(chunks):
        for d in range(1, n_buck):
            par_copy(c, d, lax.rem(mb + n_buck - d, n_buck), mb).wait_recv()
        force = parts[0, c]
        for i in range(1, n_buck):
            force = force + parts[i, c]
        out[:, c * wide:(c + 1) * wide] = force

    for m in range(1, n_elem):
        for cp in seg_copies(m, me, partner(me, m, n_elem)):
            cp.wait_send()
        cnt_copy(m, me, partner(me, m, n_elem)).wait_send()
    for c in range(chunks):
        for d in range(1, n_buck):
            par_copy(c, d, mb, lax.rem(mb + d, n_buck)).wait_send()


def local(n_elem, n_buck, node_data, eroded, bucket_map, seg_point, seg_angle):
    own, _, segs = seg_point.shape
    buckets = own * n_elem
    count = eroded.shape[0]
    elems = node_data.shape[1] // SIDES
    nfaces = SIDES * count
    wide = 512
    dma = pltpu.SemaphoreType.DMA
    points = seg_point.transpose(1, 0, 2)
    operands = (node_data, eroded[None, :], bucket_map[None, :], points, seg_angle)
    scratch = [
        (node_data.shape, F32),
        ((1, count), jnp.int32),
        ((1, node_data.shape[1]), jnp.int32),
        ((3, own, segs), F32),
        ((own, 2, segs), F32),
        ((BLOCK, BLOCK), BF16),
        ((elems, count), BF16),
        ((SIDES * 40, elems), BF16),
        ((16, nfaces), F32),
        ((buckets, nfaces), BF16),
        ((3, buckets, segs), F32),
        ((buckets, 2, segs), F32),
        ((6, buckets, segs), F32),
        ((6 * segs + 16, 4 * buckets), BF16),
        ((n_elem, 1, max(buckets, LANES)), F32),
        ((6 * segs + 16, 256), F32),
        ((6 * segs + 16, 256), F32),
        ((n_buck, nfaces // wide, 3, wide), F32),
    ]
    need = sum(math.prod(shape) * jnp.dtype(kind).itemsize for shape, kind in scratch)
    return pl.pallas_call(
        functools.partial(kernel, n_elem, n_buck),
        out_shape=jax.ShapeDtypeStruct((3, nfaces), F32),
        in_specs=[pl.BlockSpec(memory_space=pltpu.HBM)] * 5,
        out_specs=pl.BlockSpec(memory_space=pltpu.VMEM),
        scratch_shapes=[pltpu.VMEM(shape, kind) for shape, kind in scratch]
        + [
            dma((5,)),
            dma((2, n_elem - 1)),
            dma((2, n_elem - 1)),
            dma((n_elem - 1,)),
            dma((n_elem - 1,)),
            dma((nfaces // wide, n_buck - 1)),
            dma((nfaces // wide, n_buck - 1)),
        ],
        compiler_params=pltpu.CompilerParams(
            collective_id=0, has_side_effects=True,
            vmem_limit_bytes=need + 12 * 1024 * 1024,
        ),
        name="contact",
    )(*[pltpu.with_memory_space_constraint(x, pltpu.HBM) for x in operands])


def solution(mesh):
    in_specs = (
        P(None, "elem"),
        P("elem"),
        P("elem"),
        P("elem", None, "bucket"),
        P("elem", None, "bucket"),
    )
    body = functools.partial(local, mesh.shape["elem"], mesh.shape["bucket"])
    return jax.shard_map(
        body, mesh=mesh, in_specs=in_specs, out_specs=P(None, "elem"), check_vma=False
    )
```

```python
import functools
import math

import jax
import jax.numpy as jnp
from jax import lax
from jax.experimental import pallas as pl
from jax.experimental.pallas import tpu as pltpu
from jax.sharding import PartitionSpec as P

STIFFNESS = 20.0
DAMPING = 0.5
SCALE = math.sqrt(0.5 / math.log(2.0))
LANES = 128
SIDES = 6
BLOCK = SIDES * LANES
F32 = jnp.float32
BF16 = jnp.bfloat16


def split3(x):
    hi = x.astype(BF16).astype(F32)
    rest = x - hi
    mid = rest.astype(BF16).astype(F32)
    return hi, mid, rest - mid


def sin_cos(x):
    k = jnp.floor(x * 0.6366197723675814 + 0.5)
    r = x - k * 1.5703125
    r = r - k * 4.837512969970703125e-4
    r = r - k * 7.54978995489188216e-8
    z = r * r
    s = ((-1.9515295891e-4 * z + 8.3321608736e-3) * z - 1.6666654611e-1) * z * r + r
    c = ((2.443315711809948e-5 * z - 1.388731625493765e-3) * z + 4.166664568298827e-2) * z * z
    c = c - 0.5 * z + 1.0
    q = k.astype(jnp.int32) & 3
    odd = (q & 1) == 1
    sin = jnp.where(odd, c, s)
    cos = jnp.where(odd, s, c)
    sin = jnp.where(q >= 2, -sin, sin)
    cos = jnp.where((q == 1) | (q == 2), -cos, cos)
    return sin, cos


def mm(a, b, contract=((1,), (0,))):
    return lax.dot_general(a, b, (contract, ((), ())), preferred_element_type=F32)


def partner(me, m, n):
    if n & (n - 1):
        return lax.rem(me + m, n)
    to, bit = 0, 1
    while bit < n:
        to = to + bit * lax.rem(me // bit + (m // bit) % 2, 2)
        bit *= 2
    return to


def source_of(me, m, n):
    return lax.rem(me + n - m, n) if n & (n - 1) else partner(me, m, n)


def blocks_of(n, f):
    if n == 1:
        f(0)
    else:
        pl.loop(0, n)(f)


def kernel(
    n_elem, n_buck, node_any, eroded_any, bmap_any, spoint_any, sangle_any, out,
    node, eroded, bmap, perm, pick, rows, faces, onehot, table, values, seg_t, counts,
    sel0, sel1, parts,
    in_sem, seg_send, seg_recv, cnt_sem, par_send, par_recv, ready, go,
):
    me = lax.axis_index("elem")
    mb = lax.axis_index("bucket")
    buckets, segs = table.shape[1:]
    own = buckets // n_elem
    count = eroded.shape[1]
    jblocks = count // LANES
    blocks = node.shape[1] // BLOCK
    nfaces = SIDES * count
    chunks, wide = parts.shape[0], parts.shape[3]
    mesh_ids = pl.DeviceIdType.MESH

    barrier = pltpu.get_barrier_semaphore()
    for m in range(n_elem - 1, 0, -1):
        to = {"elem": partner(me, m, n_elem)}
        pl.semaphore_signal(barrier, inc=1, device_id=to, device_id_type=mesh_ids)

    leads = me == 0

    @pl.when(leads)
    def _():
        for d in range(1, n_buck):
            to = {"bucket": lax.rem(mb + d, n_buck)}
            pl.semaphore_signal(barrier, inc=1, device_id=to, device_id_type=mesh_ids)

    def held(owner):
        return table.at[:, pl.ds(pl.multiple_of(owner * own, own), own)]

    mine = pl.ds(pl.multiple_of(me * own, own), own)
    loads = [
        pltpu.make_async_copy(src, dst, in_sem.at[i])
        for i, src, dst in [
            (0, spoint_any, table.at[0:3, mine]),
            (0, sangle_any.at[:, 0], table.at[3, mine]),
            (0, sangle_any.at[:, 1], table.at[4, mine]),
            (1, eroded_any, eroded),
            (2, bmap_any, bmap),
            (3, node_any, node),
        ]
    ]
    for load in loads:
        load.start()

    col = lax.broadcasted_iota(jnp.int32, (1, BLOCK), 1)
    source = SIDES * (col & (LANES - 1)) + (col // LANES)
    for i in range(BLOCK // 256):
        r = lax.broadcasted_iota(jnp.int32, (256, BLOCK), 0) + i * 256
        perm[i * 256:(i + 1) * 256, :] = jnp.where(r == source, 1.0, 0.0).astype(BF16)

    def seg_copy(m, owner, target):
        return pltpu.make_async_remote_copy(
            src_ref=held(owner), dst_ref=held(owner),
            send_sem=seg_send, recv_sem=seg_recv.at[m - 1],
            device_id={"elem": target}, device_id_type=mesh_ids,
        )

    pltpu.make_async_copy(held(me), held(me), in_sem.at[0]).wait()
    pl.semaphore_wait(barrier, n_elem - 1 + jnp.where(leads, n_buck - 1, 0))

    for m in range(n_elem - 1, 0, -1):
        seg_copy(m, me, partner(me, m, n_elem)).start()

    @pl.when(leads)
    def _():
        for d in range(1, n_buck):
            to = {"bucket": lax.rem(mb + d, n_buck)}
            pl.semaphore_signal(ready, inc=1, device_id=to, device_id_type=mesh_ids)

    loads[3].wait()
    loads[4].wait()
    erode = eroded[...]
    high = lax.broadcasted_iota(jnp.int32, (blocks, count), 0) == erode // LANES
    low = lax.broadcasted_iota(jnp.int32, (LANES, count), 0) == lax.rem(erode, LANES)
    mask = mm(
        jnp.where(high, 1.0, 0.0).astype(BF16), jnp.where(low, 1.0, 0.0).astype(BF16), ((1,), (1,))
    )
    first = SIDES * lax.broadcasted_iota(jnp.int32, (LANES, BLOCK), 0)
    away = lax.broadcasted_iota(jnp.int32, (LANES, BLOCK), 1) - first
    spread = jnp.where((away >= 0) & (away < SIDES), 1.0, 0.0).astype(BF16)
    mask = mm(mask.astype(BF16), spread)

    chunk = min(buckets, LANES)

    def count_block(b):
        iota = lax.broadcasted_iota(jnp.int32, (chunk, LANES), 0) + b * chunk
        total = jnp.zeros((chunk, LANES), F32)
        for r in range(blocks):
            ids = jnp.where(mask[r:r + 1] > 0.5, bmap[:, r * BLOCK:(r + 1) * BLOCK], -1)
            for g in range(SIDES):
                hit = iota == ids[:, g * LANES:(g + 1) * LANES]
                total = total + jnp.where(hit, 1.0, 0.0)
        if chunk < LANES:
            total = jnp.concatenate([total, jnp.zeros((LANES - chunk, LANES), F32)], axis=0)
        sums = mm(jnp.ones((8, LANES), BF16), total.astype(BF16), ((1,), (1,)))
        at = 0 if buckets <= LANES else pl.ds(pl.multiple_of(b * LANES, LANES), LANES)
        if buckets <= LANES:
            counts[me] = sums[0:1]
        else:
            counts[me, :, at] = sums[0:1]

    blocks_of(buckets // chunk, count_block)

    def cnt_copy(at, target):
        return pltpu.make_async_remote_copy(
            src_ref=counts.at[at], dst_ref=counts.at[at],
            send_sem=cnt_sem.at[0], recv_sem=cnt_sem.at[1],
            device_id={"elem": target}, device_id_type=mesh_ids,
        )

    for m in range(n_elem - 1, 0, -1):
        cnt_copy(me, partner(me, m, n_elem)).start()

    for i in range(pick.shape[0] // 256):
        r = lax.broadcasted_iota(jnp.int32, (256, count), 0) + i * 256
        pick[i * 256:(i + 1) * 256, :] = jnp.where(r == erode, 1.0, 0.0).astype(BF16)

    loads[5].wait()
    group = 4
    for g in range(blocks // group):
        stack = []
        for i in range(g * group, (g + 1) * group):
            lanes = slice(i * BLOCK, (i + 1) * BLOCK)
            c = [node[3 * v:3 * v + 3, lanes] for v in range(8)]
            e1, e2 = c[2] - c[0], c[3] - c[1]
            r1 = jnp.concatenate([e1[1:3], e1[0:1]], axis=0)
            r2 = jnp.concatenate([e2[1:3], e2[0:1]], axis=0)
            area = 0.5 * (e1 * r2 - r1 * e2)
            centroid = 0.25 * (((c[0] + c[1]) + c[2]) + c[3])
            velocity = 0.25 * (((c[4] + c[5]) + c[6]) + c[7])
            ids = bmap[:, lanes].astype(F32)
            two = jnp.zeros((2, BLOCK), F32)
            four = jnp.zeros((4, BLOCK), F32)
            first = jnp.concatenate([centroid, area, two], axis=0)
            second = jnp.concatenate([velocity, ids, four], axis=0)
            a, b = split3(first), split3(second)
            stack += [a[0], b[0], a[1], b[1], a[2]]
        apart = mm(jnp.concatenate(stack, axis=0).astype(BF16), perm[...]).astype(BF16)
        for i in range(group):
            at = (g * group + i) * LANES
            for s in range(SIDES):
                rows[s * 40:(s + 1) * 40, at:at + LANES] = apart[
                    i * 40:(i + 1) * 40, s * LANES:(s + 1) * LANES
                ]

    @pl.when(leads)
    def _():
        pl.semaphore_wait(ready, n_buck - 1)
        for m in range(n_elem - 1, 0, -1):
            to = {"elem": partner(me, m, n_elem)}
            pl.semaphore_signal(go, inc=1, device_id=to, device_id_type=mesh_ids)

    taken = mm(rows[...], pick[...]).astype(BF16)
    stack = []
    for j in range(jblocks):
        lanes = slice(j * LANES, (j + 1) * LANES)
        stack.append(
            jnp.concatenate([taken[s * 40:(s + 1) * 40, lanes] for s in range(SIDES)], axis=1)
        )
    mixed = mm(jnp.concatenate(stack, axis=0), perm[...], ((1,), (1,)))
    for j in range(jblocks):
        t = [mixed[j * 40 + i * 8:j * 40 + i * 8 + 8] for i in range(5)]
        lanes = slice(j * BLOCK, (j + 1) * BLOCK)
        faces[0:8, lanes] = (t[0] + t[2]) + t[4]
        faces[8:16, lanes] = t[1] + t[3]

    def hot_block(b):
        for j in range(nfaces // 512):
            lanes = slice(j * 512, (j + 1) * 512)
            iota = lax.broadcasted_iota(jnp.int32, (chunk, 512), 0) + b * chunk
            hit = iota == faces[11:12, lanes].astype(jnp.int32)
            onehot[pl.ds(b * chunk, chunk), lanes] = jnp.where(hit, 1.0, 0.0).astype(BF16)

    blocks_of(buckets // chunk, hot_block)

    def unfold(owner):
        at = pl.ds(pl.multiple_of(owner * own, own), own)
        sin0, cos0 = sin_cos(table[3, at, :])
        sin1, cos1 = sin_cos(table[4, at, :])
        x, y, z = [SCALE * table[i, at, :] for i in range(3)]
        for i, v in enumerate([x, y, z, cos0 * sin1, sin0 * sin1, cos1]):
            values[i, at, :] = v

    unfold(me)
    for m in range(1, n_elem):
        owner = source_of(me, m, n_elem)
        seg_copy(m, owner, me).wait_recv()
        unfold(owner)
    cnt_copy(pl.ds(0, n_elem - 1), me).wait_recv()

    chunk = min(buckets, LANES // 2)

    def lay_out(b):
        for i in range(6):
            v = values[i, pl.ds(pl.multiple_of(b * chunk, chunk), chunk), :]
            stack = jnp.concatenate(list(split3(v)) + [jnp.zeros_like(v)], axis=0)
            lanes = pl.ds(pl.multiple_of(b * 4 * chunk, LANES), 4 * chunk)
            seg_t[i * segs:(i + 1) * segs, lanes] = stack.T.astype(BF16)

    blocks_of(buckets // chunk, lay_out)

    whole = counts[0]
    for i in range(1, n_elem):
        whole = whole + counts[i]
    stiff = (STIFFNESS / SCALE) * lax.rsqrt(jnp.maximum(whole[:, :buckets], 1.0))
    hi, mid, lo = split3(jnp.broadcast_to(stiff, (16, buckets)))
    pieces = []
    for b in range(0, buckets, chunk):
        cut = slice(b, b + chunk)
        pieces += [hi[:, cut], mid[:, cut], lo[:, cut], jnp.zeros((16, chunk), F32)]
    seg_t[6 * segs:6 * segs + 16, :] = jnp.concatenate(pieces, axis=1).astype(BF16)

    half = 256
    steps = nfaces // half

    def select(it, sel):
        hot = onehot[:, pl.ds(pl.multiple_of(it * half, half), half)]
        hot = [hot[b:b + chunk] for b in range(0, buckets, chunk) for _ in range(4)]
        sel[...] = mm(seg_t[...], jnp.concatenate(hot, axis=0))

    def forces(it, c, at, sel):
        for lt in range(half // LANES):
            g = faces[:, pl.ds(pl.multiple_of(it * half + lt * LANES, LANES), LANES)]
            cx, cy, cz, az, ax, ay, _, _, vx, vy, vz = [
                jnp.broadcast_to(g[i:i + 1], (8, LANES)) for i in range(11)
            ]
            cx, cy, cz = SCALE * cx, SCALE * cy, SCALE * cz
            damp = DAMPING / SCALE
            vx, vy, vz = damp * vx, damp * vy, damp * vz
            tile = slice(lt * LANES, (lt + 1) * LANES)
            stf = sel[6 * segs:6 * segs + 8, tile]
            acc = [jnp.zeros((8, LANES), F32) for _ in range(3)]
            for r in range(segs // 8):
                px, py, pz, nx, ny, nz = [
                    sel[q * segs + r * 8:q * segs + r * 8 + 8, tile] for q in range(6)
                ]
                ox, oy, oz = px - cx, py - cy, pz - cz
                dist = ox * ox + oy * oy + oz * oz
                depth = jnp.maximum(ox * nx + oy * ny + oz * nz, 0.0)
                proj = jnp.abs(ax * nx + ay * ny + az * nz)
                push = stf - (vx * nx + vy * ny + vz * nz)
                traction = (jnp.exp2(-dist) * depth) * (push * proj)
                for k, n in enumerate((nx, ny, nz)):
                    acc[k] = acc[k] + traction * n
            for k in range(3):
                total = jnp.sum(acc[k], axis=0, keepdims=True)
                parts[c, mb, k:k + 1, at + lt * LANES:at + (lt + 1) * LANES] = total

    def par_copy(at, who, some, target):
        return pltpu.make_async_remote_copy(
            src_ref=parts.at[at, who], dst_ref=parts.at[at, who],
            send_sem=par_send, recv_sem=par_recv.at[some],
            device_id={"bucket": target}, device_id_type=mesh_ids,
        )

    select(0, sel0)

    def step(c, carry):
        it = 2 * c
        select(it + 1, sel1)
        forces(it, c, 0, sel0)
        select(lax.rem(it + 2, steps), sel0)
        forces(it + 1, c, half, sel1)
        for d in range(1, n_buck):
            par_copy(c, mb, c // (chunks - 1), lax.rem(mb + d, n_buck)).start()
        return carry

    @pl.when(jnp.logical_not(leads))
    def _():
        pl.semaphore_wait(go, 1)

    lax.fori_loop(0, chunks, step, 0)

    others = pl.ds(0, n_buck - 1)

    def finish(c):
        force = parts[c, 0]
        for i in range(1, n_buck):
            force = force + parts[c, i]
        out[:, c * wide:(c + 1) * wide] = force

    par_copy(pl.ds(0, chunks - 1), others, 0, mb).wait_recv()
    for c in range(chunks - 1):
        finish(c)
    par_copy(pl.ds(chunks - 1, 1), others, 1, mb).wait_recv()
    finish(chunks - 1)

    rest = pl.ds(0, own * (n_elem - 1))
    pltpu.make_async_copy(table.at[:, rest], table.at[:, rest], seg_send).wait()
    cnt_copy(pl.ds(0, n_elem - 1), me).wait_send()
    par_copy(pl.ds(0, chunks), others, 0, mb).wait_send()


def local(n_elem, n_buck, node_data, eroded, bucket_map, seg_point, seg_angle):
    own, _, segs = seg_point.shape
    buckets = own * n_elem
    count = eroded.shape[0]
    elems = node_data.shape[1] // SIDES
    nfaces = SIDES * count
    wide = 512
    dma = pltpu.SemaphoreType.DMA
    points = seg_point.transpose(1, 0, 2)
    operands = (node_data, eroded[None, :], bucket_map[None, :], points, seg_angle)
    scratch = [
        (node_data.shape, F32),
        ((1, count), jnp.int32),
        ((1, node_data.shape[1]), jnp.int32),
        ((BLOCK, BLOCK), BF16),
        ((elems, count), BF16),
        ((SIDES * 40, elems), BF16),
        ((16, nfaces), F32),
        ((buckets, nfaces), BF16),
        ((5, buckets, segs), F32),
        ((6, buckets, segs), F32),
        ((6 * segs + 16, 4 * buckets), BF16),
        ((n_elem, 1, max(buckets, LANES)), F32),
        ((6 * segs + 16, 256), F32),
        ((6 * segs + 16, 256), F32),
        ((nfaces // wide, n_buck, 3, wide), F32),
    ]
    need = sum(math.prod(shape) * jnp.dtype(kind).itemsize for shape, kind in scratch)
    return pl.pallas_call(
        functools.partial(kernel, n_elem, n_buck),
        out_shape=jax.ShapeDtypeStruct((3, nfaces), F32),
        in_specs=[pl.BlockSpec(memory_space=pltpu.HBM)] * 5,
        out_specs=pl.BlockSpec(memory_space=pltpu.VMEM),
        scratch_shapes=[pltpu.VMEM(shape, kind) for shape, kind in scratch]
        + [
            dma((4,)),
            dma,
            dma((n_elem - 1,)),
            dma((2,)),
            dma,
            dma((2,)),
            pltpu.SemaphoreType.REGULAR,
            pltpu.SemaphoreType.REGULAR,
        ],
        compiler_params=pltpu.CompilerParams(
            collective_id=0, has_side_effects=True,
            vmem_limit_bytes=need + 12 * 1024 * 1024,
        ),
        name="contact",
    )(*[pltpu.with_memory_space_constraint(x, pltpu.HBM) for x in operands])


def solution(mesh):
    in_specs = (
        P(None, "elem"),
        P("elem"),
        P("elem"),
        P("elem", None, "bucket"),
        P("elem", None, "bucket"),
    )
    body = functools.partial(local, mesh.shape["elem"], mesh.shape["bucket"])
    return jax.shard_map(
        body, mesh=mesh, in_specs=in_specs, out_specs=P(None, "elem"), check_vma=False
    )
```

```python
import functools
import math

import jax
import jax.numpy as jnp
from jax import lax
from jax.experimental import pallas as pl
from jax.experimental.pallas import tpu as pltpu
from jax.sharding import PartitionSpec as P

STIFFNESS = 20.0
DAMPING = 0.5
SCALE = math.sqrt(0.5 / math.log(2.0))
LANES = 128
SIDES = 6
BLOCK = SIDES * LANES
F32 = jnp.float32
BF16 = jnp.bfloat16


def split3(x):
    hi = x.astype(BF16).astype(F32)
    rest = x - hi
    mid = rest.astype(BF16).astype(F32)
    return hi, mid, rest - mid


def sin_cos(x):
    k = jnp.floor(x * 0.6366197723675814 + 0.5)
    r = x - k * 1.5703125
    r = r - k * 4.837512969970703125e-4
    r = r - k * 7.54978995489188216e-8
    z = r * r
    s = ((-1.9515295891e-4 * z + 8.3321608736e-3) * z - 1.6666654611e-1) * z * r + r
    c = ((2.443315711809948e-5 * z - 1.388731625493765e-3) * z + 4.166664568298827e-2) * z * z
    c = c - 0.5 * z + 1.0
    q = k.astype(jnp.int32) & 3
    odd = (q & 1) == 1
    sin = jnp.where(odd, c, s)
    cos = jnp.where(odd, s, c)
    sin = jnp.where(q >= 2, -sin, sin)
    cos = jnp.where((q == 1) | (q == 2), -cos, cos)
    return sin, cos


def mm(a, b, contract=((1,), (0,))):
    return lax.dot_general(a, b, (contract, ((), ())), preferred_element_type=F32)


def partner(me, m, n):
    if n & (n - 1):
        return lax.rem(me + m, n)
    to, bit = 0, 1
    while bit < n:
        to = to + bit * lax.rem(me // bit + (m // bit) % 2, 2)
        bit *= 2
    return to


def source_of(me, m, n):
    return lax.rem(me + n - m, n) if n & (n - 1) else partner(me, m, n)


def other(me, u):
    return u + jnp.where(u >= me, 1, 0)


def blocks_of(n, f):
    if n == 1:
        f(0)
    else:
        pl.loop(0, n)(f)


def kernel(
    n_elem, n_buck, node_any, eroded_any, bmap_any, spoint_any, sangle_any, out,
    node, eroded, bmap, perm, spread, pick, rows, faces, onehot, table, values, seg_t, counts,
    sel0, sel1, parts,
    in_sem, seg_send, seg_recv, cnt_sem, par_send, par_recv, ready, go,
):
    me = lax.axis_index("elem")
    mb = lax.axis_index("bucket")
    buckets, segs = table.shape[1:]
    own = buckets // n_elem
    count = eroded.shape[1]
    jblocks = count // LANES
    blocks = node.shape[1] // BLOCK
    nfaces = SIDES * count
    chunks, wide = parts.shape[0], parts.shape[3]
    mesh_ids = pl.DeviceIdType.MESH

    barrier = pltpu.get_barrier_semaphore()
    for u in range(n_elem - 1):
        to = {"elem": other(me, u)}
        pl.semaphore_signal(barrier, inc=1, device_id=to, device_id_type=mesh_ids)

    leads = me == 0

    @pl.when(leads)
    def _():
        for d in range(1, n_buck):
            to = {"bucket": lax.rem(mb + d, n_buck)}
            pl.semaphore_signal(barrier, inc=1, device_id=to, device_id_type=mesh_ids)

    def held(owner):
        return table.at[:, pl.ds(pl.multiple_of(owner * own, own), own)]

    mine = pl.ds(pl.multiple_of(me * own, own), own)
    loads = [
        pltpu.make_async_copy(src, dst, in_sem.at[i])
        for i, src, dst in [
            (0, spoint_any, table.at[0:3, mine]),
            (0, sangle_any.at[:, 0], table.at[3, mine]),
            (0, sangle_any.at[:, 1], table.at[4, mine]),
            (1, eroded_any, eroded),
            (2, bmap_any, bmap),
            (3, node_any, node),
        ]
    ]
    for load in loads:
        load.start()

    col = lax.broadcasted_iota(jnp.int32, (1, BLOCK), 1)
    source = SIDES * (col & (LANES - 1)) + (col // LANES)
    for i in range(BLOCK // 256):
        r = lax.broadcasted_iota(jnp.int32, (256, BLOCK), 0) + i * 256
        perm[i * 256:(i + 1) * 256, :] = jnp.where(r == source, 1.0, 0.0).astype(BF16)

    first = SIDES * lax.broadcasted_iota(jnp.int32, (LANES, BLOCK), 0)
    away = lax.broadcasted_iota(jnp.int32, (LANES, BLOCK), 1) - first
    spread[...] = jnp.where((away >= 0) & (away < SIDES), 1.0, 0.0).astype(BF16)

    def seg_copy(owner, target):
        return pltpu.make_async_remote_copy(
            src_ref=held(owner), dst_ref=held(owner),
            send_sem=seg_send, recv_sem=seg_recv.at[owner - jnp.where(owner > target, 1, 0)],
            device_id={"elem": target}, device_id_type=mesh_ids,
        )

    chunk = min(buckets, LANES)

    def tally():
        loads[3].wait()
        loads[4].wait()
        erode = eroded[...]
        high = lax.broadcasted_iota(jnp.int32, (blocks, count), 0) == erode // LANES
        low = lax.broadcasted_iota(jnp.int32, (LANES, count), 0) == lax.rem(erode, LANES)
        mask = mm(
            jnp.where(high, 1.0, 0.0).astype(BF16), jnp.where(low, 1.0, 0.0).astype(BF16), ((1,), (1,))
        )
        mask = mm(mask.astype(BF16), spread[...])

        def count_block(b):
            iota = lax.broadcasted_iota(jnp.int32, (chunk, LANES), 0) + b * chunk
            total = jnp.zeros((chunk, LANES), F32)
            for r in range(blocks):
                ids = jnp.where(mask[r:r + 1] > 0.5, bmap[:, r * BLOCK:(r + 1) * BLOCK], -1)
                for g in range(SIDES):
                    hit = iota == ids[:, g * LANES:(g + 1) * LANES]
                    total = total + jnp.where(hit, 1.0, 0.0)
            if chunk < LANES:
                total = jnp.concatenate([total, jnp.zeros((LANES - chunk, LANES), F32)], axis=0)
            sums = mm(jnp.ones((8, LANES), BF16), total.astype(BF16), ((1,), (1,)))
            at = 0 if buckets <= LANES else pl.ds(pl.multiple_of(b * LANES, LANES), LANES)
            if buckets <= LANES:
                counts[me] = sums[0:1]
            else:
                counts[me, :, at] = sums[0:1]

        blocks_of(buckets // chunk, count_block)

    def gather():
        for i in range(pick.shape[0] // 256):
            r = lax.broadcasted_iota(jnp.int32, (256, count), 0) + i * 256
            pick[i * 256:(i + 1) * 256, :] = jnp.where(r == eroded[...], 1.0, 0.0).astype(BF16)

        loads[5].wait()
        group = 4
        for g in range(blocks // group):
            stack = []
            for i in range(g * group, (g + 1) * group):
                lanes = slice(i * BLOCK, (i + 1) * BLOCK)
                c = [node[3 * v:3 * v + 3, lanes] for v in range(8)]
                e1, e2 = c[2] - c[0], c[3] - c[1]
                r1 = jnp.concatenate([e1[1:3], e1[0:1]], axis=0)
                r2 = jnp.concatenate([e2[1:3], e2[0:1]], axis=0)
                area = 0.5 * (e1 * r2 - r1 * e2)
                centroid = 0.25 * (((c[0] + c[1]) + c[2]) + c[3])
                velocity = 0.25 * (((c[4] + c[5]) + c[6]) + c[7])
                ids = bmap[:, lanes].astype(F32)
                two = jnp.zeros((2, BLOCK), F32)
                four = jnp.zeros((4, BLOCK), F32)
                first = jnp.concatenate([centroid, area, two], axis=0)
                second = jnp.concatenate([velocity, ids, four], axis=0)
                a, b = split3(first), split3(second)
                stack += [a[0], b[0], a[1], b[1], a[2]]
            apart = mm(jnp.concatenate(stack, axis=0).astype(BF16), perm[...]).astype(BF16)
            for i in range(group):
                at = (g * group + i) * LANES
                for s in range(SIDES):
                    rows[s * 40:(s + 1) * 40, at:at + LANES] = apart[
                        i * 40:(i + 1) * 40, s * LANES:(s + 1) * LANES
                    ]

        taken = mm(rows[...], pick[...]).astype(BF16)
        stack = []
        for j in range(jblocks):
            lanes = slice(j * LANES, (j + 1) * LANES)
            stack.append(
                jnp.concatenate([taken[s * 40:(s + 1) * 40, lanes] for s in range(SIDES)], axis=1)
            )
        mixed = mm(jnp.concatenate(stack, axis=0), perm[...], ((1,), (1,)))
        for j in range(jblocks):
            t = [mixed[j * 40 + i * 8:j * 40 + i * 8 + 8] for i in range(5)]
            lanes = slice(j * BLOCK, (j + 1) * BLOCK)
            faces[0:8, lanes] = (t[0] + t[2]) + t[4]
            faces[8:16, lanes] = t[1] + t[3]

        def hot_block(b):
            for j in range(nfaces // 512):
                lanes = slice(j * 512, (j + 1) * 512)
                iota = lax.broadcasted_iota(jnp.int32, (chunk, 512), 0) + b * chunk
                hit = iota == faces[11:12, lanes].astype(jnp.int32)
                onehot[pl.ds(b * chunk, chunk), lanes] = jnp.where(hit, 1.0, 0.0).astype(BF16)

        blocks_of(buckets // chunk, hot_block)

    @pl.when(leads)
    def _():
        tally()
        gather()

    pltpu.make_async_copy(held(me), held(me), in_sem.at[0]).wait()
    pl.semaphore_wait(barrier, n_elem - 1 + jnp.where(leads, n_buck - 1, 0))

    for u in range(n_elem - 1):
        seg_copy(me, other(me, u)).start()

    @pl.when(leads)
    def _():
        for d in range(1, n_buck):
            to = {"bucket": lax.rem(mb + d, n_buck)}
            pl.semaphore_signal(ready, inc=1, device_id=to, device_id_type=mesh_ids)

    def cnt_copy(at, target):
        return pltpu.make_async_remote_copy(
            src_ref=counts.at[at], dst_ref=counts.at[at],
            send_sem=cnt_sem.at[0], recv_sem=cnt_sem.at[1],
            device_id={"elem": target}, device_id_type=mesh_ids,
        )

    @pl.when(jnp.logical_not(leads))
    def _():
        tally()

    for u in range(n_elem - 1):
        cnt_copy(me, other(me, u)).start()

    @pl.when(jnp.logical_not(leads))
    def _():
        gather()

    @pl.when(leads)
    def _():
        pl.semaphore_wait(ready, n_buck - 1)
        for u in range(n_elem - 1):
            to = {"elem": other(me, u)}
            pl.semaphore_signal(go, inc=1, device_id=to, device_id_type=mesh_ids)

    def unfold(owner):
        at = pl.ds(pl.multiple_of(owner * own, own), own)
        sin0, cos0 = sin_cos(table[3, at, :])
        sin1, cos1 = sin_cos(table[4, at, :])
        x, y, z = [SCALE * table[i, at, :] for i in range(3)]
        for i, v in enumerate([x, y, z, cos0 * sin1, sin0 * sin1, cos1]):
            values[i, at, :] = v

    unfold(me)
    for m in range(1, n_elem):
        owner = source_of(me, m, n_elem)
        seg_copy(owner, me).wait_recv()
        unfold(owner)
    cnt_copy(pl.ds(0, n_elem - 1), me).wait_recv()

    chunk = min(buckets, LANES // 2)

    def lay_out(b):
        for i in range(6):
            v = values[i, pl.ds(pl.multiple_of(b * chunk, chunk), chunk), :]
            stack = jnp.concatenate(list(split3(v)) + [jnp.zeros_like(v)], axis=0)
            lanes = pl.ds(pl.multiple_of(b * 4 * chunk, LANES), 4 * chunk)
            seg_t[i * segs:(i + 1) * segs, lanes] = stack.T.astype(BF16)

    blocks_of(buckets // chunk, lay_out)

    whole = counts[0]
    for i in range(1, n_elem):
        whole = whole + counts[i]
    stiff = (STIFFNESS / SCALE) * lax.rsqrt(jnp.maximum(whole[:, :buckets], 1.0))
    hi, mid, lo = split3(jnp.broadcast_to(stiff, (16, buckets)))
    pieces = []
    for b in range(0, buckets, chunk):
        cut = slice(b, b + chunk)
        pieces += [hi[:, cut], mid[:, cut], lo[:, cut], jnp.zeros((16, chunk), F32)]
    seg_t[6 * segs:6 * segs + 16, :] = jnp.concatenate(pieces, axis=1).astype(BF16)

    half = 256
    steps = nfaces // half

    def select(it, sel):
        hot = onehot[:, pl.ds(pl.multiple_of(it * half, half), half)]
        hot = [hot[b:b + chunk] for b in range(0, buckets, chunk) for _ in range(4)]
        sel[...] = mm(seg_t[...], jnp.concatenate(hot, axis=0))

    def forces(it, c, at, sel):
        for lt in range(half // LANES):
            g = faces[:, pl.ds(pl.multiple_of(it * half + lt * LANES, LANES), LANES)]
            cx, cy, cz, az, ax, ay, _, _, vx, vy, vz = [
                jnp.broadcast_to(g[i:i + 1], (8, LANES)) for i in range(11)
            ]
            cx, cy, cz = SCALE * cx, SCALE * cy, SCALE * cz
            damp = DAMPING / SCALE
            vx, vy, vz = damp * vx, damp * vy, damp * vz
            tile = slice(lt * LANES, (lt + 1) * LANES)
            stf = sel[6 * segs:6 * segs + 8, tile]
            acc = [jnp.zeros((8, LANES), F32) for _ in range(3)]
            for r in range(segs // 8):
                px, py, pz, nx, ny, nz = [
                    sel[q * segs + r * 8:q * segs + r * 8 + 8, tile] for q in range(6)
                ]
                ox, oy, oz = px - cx, py - cy, pz - cz
                dist = ox * ox + oy * oy + oz * oz
                depth = jnp.maximum(ox * nx + oy * ny + oz * nz, 0.0)
                proj = jnp.abs(ax * nx + ay * ny + az * nz)
                push = stf - (vx * nx + vy * ny + vz * nz)
                traction = (jnp.exp2(-dist) * depth) * (push * proj)
                for k, n in enumerate((nx, ny, nz)):
                    acc[k] = acc[k] + traction * n
            for k in range(3):
                total = jnp.sum(acc[k], axis=0, keepdims=True)
                parts[c, mb, k:k + 1, at + lt * LANES:at + (lt + 1) * LANES] = total

    def par_copy(at, who, some, target):
        return pltpu.make_async_remote_copy(
            src_ref=parts.at[at, who], dst_ref=parts.at[at, who],
            send_sem=par_send, recv_sem=par_recv.at[some],
            device_id={"bucket": target}, device_id_type=mesh_ids,
        )

    select(0, sel0)

    def step(c, carry):
        it = 2 * c
        select(it + 1, sel1)
        forces(it, c, 0, sel0)
        select(lax.rem(it + 2, steps), sel0)
        forces(it + 1, c, half, sel1)
        for m in sorted(range(1, n_buck), key=lambda m: m == 1):
            par_copy(c, mb, c // (chunks - 1), partner(mb, m, n_buck)).start()
        return carry

    @pl.when(jnp.logical_not(leads))
    def _():
        pl.semaphore_wait(go, 1)

    lax.fori_loop(0, chunks, step, 0)

    others = pl.ds(0, n_buck - 1)

    def finish(c):
        force = parts[c, 0]
        for i in range(1, n_buck):
            force = force + parts[c, i]
        out[:, c * wide:(c + 1) * wide] = force

    par_copy(pl.ds(0, chunks - 1), others, 0, mb).wait_recv()
    for c in range(chunks - 1):
        finish(c)
    par_copy(pl.ds(chunks - 1, 1), others, 1, mb).wait_recv()
    finish(chunks - 1)

    rest = pl.ds(0, own * (n_elem - 1))
    pltpu.make_async_copy(table.at[:, rest], table.at[:, rest], seg_send).wait()
    cnt_copy(pl.ds(0, n_elem - 1), me).wait_send()
    par_copy(pl.ds(0, chunks), others, 0, mb).wait_send()


def local(n_elem, n_buck, node_data, eroded, bucket_map, seg_point, seg_angle):
    own, _, segs = seg_point.shape
    buckets = own * n_elem
    count = eroded.shape[0]
    elems = node_data.shape[1] // SIDES
    nfaces = SIDES * count
    wide = 512
    dma = pltpu.SemaphoreType.DMA
    points = seg_point.transpose(1, 0, 2)
    operands = (node_data, eroded[None, :], bucket_map[None, :], points, seg_angle)
    scratch = [
        (node_data.shape, F32),
        ((1, count), jnp.int32),
        ((1, node_data.shape[1]), jnp.int32),
        ((BLOCK, BLOCK), BF16),
        ((LANES, BLOCK), BF16),
        ((elems, count), BF16),
        ((SIDES * 40, elems), BF16),
        ((16, nfaces), F32),
        ((buckets, nfaces), BF16),
        ((5, buckets, segs), F32),
        ((6, buckets, segs), F32),
        ((6 * segs + 16, 4 * buckets), BF16),
        ((n_elem, 1, max(buckets, LANES)), F32),
        ((6 * segs + 16, 256), F32),
        ((6 * segs + 16, 256), F32),
        ((nfaces // wide, n_buck, 3, wide), F32),
    ]
    need = sum(math.prod(shape) * jnp.dtype(kind).itemsize for shape, kind in scratch)
    return pl.pallas_call(
        functools.partial(kernel, n_elem, n_buck),
        out_shape=jax.ShapeDtypeStruct((3, nfaces), F32),
        in_specs=[pl.BlockSpec(memory_space=pltpu.HBM)] * 5,
        out_specs=pl.BlockSpec(memory_space=pltpu.VMEM),
        scratch_shapes=[pltpu.VMEM(shape, kind) for shape, kind in scratch]
        + [
            dma((4,)),
            dma,
            dma((n_elem - 1,)),
            dma((2,)),
            dma,
            dma((2,)),
            pltpu.SemaphoreType.REGULAR,
            pltpu.SemaphoreType.REGULAR,
        ],
        compiler_params=pltpu.CompilerParams(
            collective_id=0, has_side_effects=True,
            vmem_limit_bytes=need + 12 * 1024 * 1024,
        ),
        name="contact",
    )(*[pltpu.with_memory_space_constraint(x, pltpu.HBM) for x in operands])


def solution(mesh):
    in_specs = (
        P(None, "elem"),
        P("elem"),
        P("elem"),
        P("elem", None, "bucket"),
        P("elem", None, "bucket"),
    )
    body = functools.partial(local, mesh.shape["elem"], mesh.shape["bucket"])
    return jax.shard_map(
        body, mesh=mesh, in_specs=in_specs, out_specs=P(None, "elem"), check_vma=False
    )
```

```python
import functools
import math

import jax
import jax.numpy as jnp
from jax import lax
from jax.experimental import pallas as pl
from jax.experimental.pallas import tpu as pltpu
from jax.sharding import PartitionSpec as P

STIFFNESS = 20.0
DAMPING = 0.5
SCALE = math.sqrt(0.5 / math.log(2.0))
LANES = 128
SIDES = 6
BLOCK = SIDES * LANES
F32 = jnp.float32
BF16 = jnp.bfloat16


def split3(x):
    hi = x.astype(BF16).astype(F32)
    rest = x - hi
    mid = rest.astype(BF16).astype(F32)
    return hi, mid, rest - mid


def sin_cos(x):
    k = jnp.floor(x * 0.6366197723675814 + 0.5)
    r = x - k * 1.5703125
    r = r - k * 4.837512969970703125e-4
    r = r - k * 7.54978995489188216e-8
    z = r * r
    s = ((-1.9515295891e-4 * z + 8.3321608736e-3) * z - 1.6666654611e-1) * z * r + r
    c = ((2.443315711809948e-5 * z - 1.388731625493765e-3) * z + 4.166664568298827e-2) * z * z
    c = c - 0.5 * z + 1.0
    q = k.astype(jnp.int32) & 3
    odd = (q & 1) == 1
    sin = jnp.where(odd, c, s)
    cos = jnp.where(odd, s, c)
    sin = jnp.where(q >= 2, -sin, sin)
    cos = jnp.where((q == 1) | (q == 2), -cos, cos)
    return sin, cos


def mm(a, b, contract=((1,), (0,))):
    return lax.dot_general(a, b, (contract, ((), ())), preferred_element_type=F32)


def partner(me, m, n):
    if n & (n - 1):
        return lax.rem(me + m, n)
    to, bit = 0, 1
    while bit < n:
        to = to + bit * lax.rem(me // bit + (m // bit) % 2, 2)
        bit *= 2
    return to


def source_of(me, m, n):
    return lax.rem(me + n - m, n) if n & (n - 1) else partner(me, m, n)


def other(me, u):
    return u + jnp.where(u >= me, 1, 0)


def blocks_of(n, f):
    if n == 1:
        f(0)
    else:
        pl.loop(0, n)(f)


def kernel(
    n_elem, n_buck, node_any, eroded_any, bmap_any, spoint_any, sangle_any, out,
    node, eroded, bmap, perm, spread, pick, rows, faces, onehot, table, values, seg_t, counts,
    sel0, sel1, parts,
    in_sem, seg_send, seg_recv, cnt_sem, par_send, par_recv, ready, go,
):
    me = lax.axis_index("elem")
    mb = lax.axis_index("bucket")
    buckets, segs = table.shape[1:]
    own = buckets // n_elem
    count = eroded.shape[1]
    jblocks = count // LANES
    blocks = node.shape[1] // BLOCK
    nfaces = SIDES * count
    chunks, wide = parts.shape[0], parts.shape[3]
    mesh_ids = pl.DeviceIdType.MESH

    barrier = pltpu.get_barrier_semaphore()
    for u in range(n_elem - 1):
        to = {"elem": other(me, u)}
        pl.semaphore_signal(barrier, inc=1, device_id=to, device_id_type=mesh_ids)

    leads = me == 0

    @pl.when(leads)
    def _():
        for d in range(1, n_buck):
            to = {"bucket": lax.rem(mb + d, n_buck)}
            pl.semaphore_signal(barrier, inc=1, device_id=to, device_id_type=mesh_ids)

    def held(owner):
        return table.at[:, pl.ds(pl.multiple_of(owner * own, own), own)]

    mine = pl.ds(pl.multiple_of(me * own, own), own)
    loads = [
        pltpu.make_async_copy(src, dst, in_sem.at[i])
        for i, src, dst in [
            (0, spoint_any, table.at[0:3, mine]),
            (0, sangle_any.at[:, 0], table.at[3, mine]),
            (0, sangle_any.at[:, 1], table.at[4, mine]),
            (1, eroded_any, eroded),
            (2, bmap_any, bmap),
            (3, node_any, node),
        ]
    ]
    for load in loads:
        load.start()

    col = lax.broadcasted_iota(jnp.int32, (1, BLOCK), 1)
    source = SIDES * (col & (LANES - 1)) + (col // LANES)
    for i in range(BLOCK // 256):
        r = lax.broadcasted_iota(jnp.int32, (256, BLOCK), 0) + i * 256
        perm[i * 256:(i + 1) * 256, :] = jnp.where(r == source, 1.0, 0.0).astype(BF16)

    first = SIDES * lax.broadcasted_iota(jnp.int32, (LANES, BLOCK), 0)
    away = lax.broadcasted_iota(jnp.int32, (LANES, BLOCK), 1) - first
    spread[...] = jnp.where((away >= 0) & (away < SIDES), 1.0, 0.0).astype(BF16)

    def seg_copy(owner, target):
        return pltpu.make_async_remote_copy(
            src_ref=held(owner), dst_ref=held(owner),
            send_sem=seg_send, recv_sem=seg_recv.at[owner - jnp.where(owner > target, 1, 0)],
            device_id={"elem": target}, device_id_type=mesh_ids,
        )

    chunk = min(buckets, LANES)

    def tally():
        loads[3].wait()
        loads[4].wait()
        erode = eroded[...]
        high = lax.broadcasted_iota(jnp.int32, (blocks, count), 0) == erode // LANES
        low = lax.broadcasted_iota(jnp.int32, (LANES, count), 0) == lax.rem(erode, LANES)
        mask = mm(
            jnp.where(high, 1.0, 0.0).astype(BF16), jnp.where(low, 1.0, 0.0).astype(BF16), ((1,), (1,))
        )
        mask = mm(mask.astype(BF16), spread[...])

        def count_block(b):
            iota = lax.broadcasted_iota(jnp.int32, (chunk, LANES), 0) + b * chunk
            total = jnp.zeros((chunk, LANES), F32)
            for r in range(blocks):
                ids = jnp.where(mask[r:r + 1] > 0.5, bmap[:, r * BLOCK:(r + 1) * BLOCK], -1)
                for g in range(SIDES):
                    hit = iota == ids[:, g * LANES:(g + 1) * LANES]
                    total = total + jnp.where(hit, 1.0, 0.0)
            if chunk < LANES:
                total = jnp.concatenate([total, jnp.zeros((LANES - chunk, LANES), F32)], axis=0)
            sums = mm(jnp.ones((8, LANES), BF16), total.astype(BF16), ((1,), (1,)))
            at = 0 if buckets <= LANES else pl.ds(pl.multiple_of(b * LANES, LANES), LANES)
            if buckets <= LANES:
                counts[me] = sums[0:1]
            else:
                counts[me, :, at] = sums[0:1]

        blocks_of(buckets // chunk, count_block)

    def gather():
        for i in range(pick.shape[0] // 256):
            r = lax.broadcasted_iota(jnp.int32, (256, count), 0) + i * 256
            pick[i * 256:(i + 1) * 256, :] = jnp.where(r == eroded[...], 1.0, 0.0).astype(BF16)

        loads[5].wait()
        group = 4
        for g in range(blocks // group):
            stack = []
            for i in range(g * group, (g + 1) * group):
                lanes = slice(i * BLOCK, (i + 1) * BLOCK)
                c = [node[3 * v:3 * v + 3, lanes] for v in range(8)]
                e1, e2 = c[2] - c[0], c[3] - c[1]
                r1 = jnp.concatenate([e1[1:3], e1[0:1]], axis=0)
                r2 = jnp.concatenate([e2[1:3], e2[0:1]], axis=0)
                area = 0.5 * (e1 * r2 - r1 * e2)
                centroid = 0.25 * (((c[0] + c[1]) + c[2]) + c[3])
                velocity = 0.25 * (((c[4] + c[5]) + c[6]) + c[7])
                ids = bmap[:, lanes].astype(F32)
                two = jnp.zeros((2, BLOCK), F32)
                four = jnp.zeros((4, BLOCK), F32)
                first = jnp.concatenate([centroid, area, two], axis=0)
                second = jnp.concatenate([velocity, ids, four], axis=0)
                a, b = split3(first), split3(second)
                stack += [a[0], b[0], a[1], b[1], a[2]]
            apart = mm(jnp.concatenate(stack, axis=0).astype(BF16), perm[...]).astype(BF16)
            for i in range(group):
                at = (g * group + i) * LANES
                for s in range(SIDES):
                    rows[s * 40:(s + 1) * 40, at:at + LANES] = apart[
                        i * 40:(i + 1) * 40, s * LANES:(s + 1) * LANES
                    ]

        taken = mm(rows[...], pick[...]).astype(BF16)
        stack = []
        for j in range(jblocks):
            lanes = slice(j * LANES, (j + 1) * LANES)
            stack.append(
                jnp.concatenate([taken[s * 40:(s + 1) * 40, lanes] for s in range(SIDES)], axis=1)
            )
        mixed = mm(jnp.concatenate(stack, axis=0), perm[...], ((1,), (1,)))
        for j in range(jblocks):
            t = [mixed[j * 40 + i * 8:j * 40 + i * 8 + 8] for i in range(5)]
            lanes = slice(j * BLOCK, (j + 1) * BLOCK)
            faces[0:8, lanes] = (t[0] + t[2]) + t[4]
            faces[8:16, lanes] = t[1] + t[3]

        def hot_block(b):
            for j in range(nfaces // 512):
                lanes = slice(j * 512, (j + 1) * 512)
                iota = lax.broadcasted_iota(jnp.int32, (chunk, 512), 0) + b * chunk
                hit = iota == faces[11:12, lanes].astype(jnp.int32)
                onehot[pl.ds(b * chunk, chunk), lanes] = jnp.where(hit, 1.0, 0.0).astype(BF16)

        blocks_of(buckets // chunk, hot_block)

    @pl.when(leads)
    def _():
        tally()
        gather()

    pltpu.make_async_copy(held(me), held(me), in_sem.at[0]).wait()
    pl.semaphore_wait(barrier, n_elem - 1 + jnp.where(leads, n_buck - 1, 0))

    seg_copy(me, other(me, 0)).start()

    @pl.when(leads)
    def _():
        for d in range(1, n_buck):
            to = {"bucket": lax.rem(mb + d, n_buck)}
            pl.semaphore_signal(ready, inc=1, device_id=to, device_id_type=mesh_ids)

    def cnt_copy(at, target):
        return pltpu.make_async_remote_copy(
            src_ref=counts.at[at], dst_ref=counts.at[at],
            send_sem=cnt_sem.at[0], recv_sem=cnt_sem.at[1],
            device_id={"elem": target}, device_id_type=mesh_ids,
        )

    @pl.when(jnp.logical_not(leads))
    def _():
        tally()

    for u in range(n_elem - 1):
        cnt_copy(me, other(me, u)).start()
    for u in range(1, n_elem - 1):
        seg_copy(me, other(me, u)).start()

    @pl.when(jnp.logical_not(leads))
    def _():
        gather()

    @pl.when(leads)
    def _():
        pl.semaphore_wait(ready, n_buck - 1)
        for u in range(n_elem - 1):
            to = {"elem": other(me, u)}
            pl.semaphore_signal(go, inc=1, device_id=to, device_id_type=mesh_ids)

    def unfold(owner):
        at = pl.ds(pl.multiple_of(owner * own, own), own)
        sin0, cos0 = sin_cos(table[3, at, :])
        sin1, cos1 = sin_cos(table[4, at, :])
        x, y, z = [SCALE * table[i, at, :] for i in range(3)]
        for i, v in enumerate([x, y, z, cos0 * sin1, sin0 * sin1, cos1]):
            values[i, at, :] = v

    unfold(me)
    for m in range(1, n_elem):
        owner = source_of(me, m, n_elem)
        seg_copy(owner, me).wait_recv()
        unfold(owner)
    cnt_copy(pl.ds(0, n_elem - 1), me).wait_recv()

    chunk = min(buckets, LANES // 2)

    def lay_out(b):
        for i in range(6):
            v = values[i, pl.ds(pl.multiple_of(b * chunk, chunk), chunk), :]
            stack = jnp.concatenate(list(split3(v)) + [jnp.zeros_like(v)], axis=0)
            lanes = pl.ds(pl.multiple_of(b * 4 * chunk, LANES), 4 * chunk)
            seg_t[i * segs:(i + 1) * segs, lanes] = stack.T.astype(BF16)

    blocks_of(buckets // chunk, lay_out)

    whole = counts[0]
    for i in range(1, n_elem):
        whole = whole + counts[i]
    stiff = (STIFFNESS / SCALE) * lax.rsqrt(jnp.maximum(whole[:, :buckets], 1.0))
    hi, mid, lo = split3(jnp.broadcast_to(stiff, (16, buckets)))
    pieces = []
    for b in range(0, buckets, chunk):
        cut = slice(b, b + chunk)
        pieces += [hi[:, cut], mid[:, cut], lo[:, cut], jnp.zeros((16, chunk), F32)]
    seg_t[6 * segs:6 * segs + 16, :] = jnp.concatenate(pieces, axis=1).astype(BF16)

    half = 256
    steps = nfaces // half

    def select(it, sel):
        hot = onehot[:, pl.ds(pl.multiple_of(it * half, half), half)]
        hot = [hot[b:b + chunk] for b in range(0, buckets, chunk) for _ in range(4)]
        sel[...] = mm(seg_t[...], jnp.concatenate(hot, axis=0))

    def forces(it, c, at, sel):
        for lt in range(half // LANES):
            g = faces[:, pl.ds(pl.multiple_of(it * half + lt * LANES, LANES), LANES)]
            cx, cy, cz, az, ax, ay, _, _, vx, vy, vz = [
                jnp.broadcast_to(g[i:i + 1], (8, LANES)) for i in range(11)
            ]
            cx, cy, cz = SCALE * cx, SCALE * cy, SCALE * cz
            damp = DAMPING / SCALE
            vx, vy, vz = damp * vx, damp * vy, damp * vz
            tile = slice(lt * LANES, (lt + 1) * LANES)
            stf = sel[6 * segs:6 * segs + 8, tile]
            acc = [jnp.zeros((8, LANES), F32) for _ in range(3)]
            for r in range(segs // 8):
                px, py, pz, nx, ny, nz = [
                    sel[q * segs + r * 8:q * segs + r * 8 + 8, tile] for q in range(6)
                ]
                ox, oy, oz = px - cx, py - cy, pz - cz
                dist = ox * ox + oy * oy + oz * oz
                depth = jnp.maximum(ox * nx + oy * ny + oz * nz, 0.0)
                proj = jnp.abs(ax * nx + ay * ny + az * nz)
                push = stf - (vx * nx + vy * ny + vz * nz)
                traction = (jnp.exp2(-dist) * depth) * (push * proj)
                for k, n in enumerate((nx, ny, nz)):
                    acc[k] = acc[k] + traction * n
            for k in range(3):
                total = jnp.sum(acc[k], axis=0, keepdims=True)
                parts[c, mb, k:k + 1, at + lt * LANES:at + (lt + 1) * LANES] = total

    def par_copy(at, who, some, target):
        return pltpu.make_async_remote_copy(
            src_ref=parts.at[at, who], dst_ref=parts.at[at, who],
            send_sem=par_send, recv_sem=par_recv.at[some],
            device_id={"bucket": target}, device_id_type=mesh_ids,
        )

    select(0, sel0)

    def step(c, carry):
        it = 2 * c
        select(it + 1, sel1)
        forces(it, c, 0, sel0)
        select(lax.rem(it + 2, steps), sel0)
        forces(it + 1, c, half, sel1)
        for m in sorted(range(1, n_buck), key=lambda m: m == 1):
            par_copy(c, mb, c // (chunks - 1), partner(mb, m, n_buck)).start()
        return carry

    @pl.when(jnp.logical_not(leads))
    def _():
        pl.semaphore_wait(go, 1)

    lax.fori_loop(0, chunks, step, 0)

    others = pl.ds(0, n_buck - 1)

    def finish(c):
        force = parts[c, 0]
        for i in range(1, n_buck):
            force = force + parts[c, i]
        out[:, c * wide:(c + 1) * wide] = force

    par_copy(pl.ds(0, chunks - 1), others, 0, mb).wait_recv()
    for c in range(chunks - 1):
        finish(c)
    par_copy(pl.ds(chunks - 1, 1), others, 1, mb).wait_recv()
    finish(chunks - 1)

    rest = pl.ds(0, own * (n_elem - 1))
    pltpu.make_async_copy(table.at[:, rest], table.at[:, rest], seg_send).wait()
    cnt_copy(pl.ds(0, n_elem - 1), me).wait_send()
    par_copy(pl.ds(0, chunks), others, 0, mb).wait_send()


def local(n_elem, n_buck, node_data, eroded, bucket_map, seg_point, seg_angle):
    own, _, segs = seg_point.shape
    buckets = own * n_elem
    count = eroded.shape[0]
    elems = node_data.shape[1] // SIDES
    nfaces = SIDES * count
    wide = 512
    dma = pltpu.SemaphoreType.DMA
    points = seg_point.transpose(1, 0, 2)
    operands = (node_data, eroded[None, :], bucket_map[None, :], points, seg_angle)
    scratch = [
        (node_data.shape, F32),
        ((1, count), jnp.int32),
        ((1, node_data.shape[1]), jnp.int32),
        ((BLOCK, BLOCK), BF16),
        ((LANES, BLOCK), BF16),
        ((elems, count), BF16),
        ((SIDES * 40, elems), BF16),
        ((16, nfaces), F32),
        ((buckets, nfaces), BF16),
        ((5, buckets, segs), F32),
        ((6, buckets, segs), F32),
        ((6 * segs + 16, 4 * buckets), BF16),
        ((n_elem, 1, max(buckets, LANES)), F32),
        ((6 * segs + 16, 256), F32),
        ((6 * segs + 16, 256), F32),
        ((nfaces // wide, n_buck, 3, wide), F32),
    ]
    need = sum(math.prod(shape) * jnp.dtype(kind).itemsize for shape, kind in scratch)
    return pl.pallas_call(
        functools.partial(kernel, n_elem, n_buck),
        out_shape=jax.ShapeDtypeStruct((3, nfaces), F32),
        in_specs=[pl.BlockSpec(memory_space=pltpu.HBM)] * 5,
        out_specs=pl.BlockSpec(memory_space=pltpu.VMEM),
        scratch_shapes=[pltpu.VMEM(shape, kind) for shape, kind in scratch]
        + [
            dma((4,)),
            dma,
            dma((n_elem - 1,)),
            dma((2,)),
            dma,
            dma((2,)),
            pltpu.SemaphoreType.REGULAR,
            pltpu.SemaphoreType.REGULAR,
        ],
        compiler_params=pltpu.CompilerParams(
            collective_id=0, has_side_effects=True,
            vmem_limit_bytes=need + 12 * 1024 * 1024,
        ),
        name="contact",
    )(*[pltpu.with_memory_space_constraint(x, pltpu.HBM) for x in operands])


def solution(mesh):
    in_specs = (
        P(None, "elem"),
        P("elem"),
        P("elem"),
        P("elem", None, "bucket"),
        P("elem", None, "bucket"),
    )
    body = functools.partial(local, mesh.shape["elem"], mesh.shape["bucket"])
    return jax.shard_map(
        body, mesh=mesh, in_specs=in_specs, out_specs=P(None, "elem"), check_vma=False
    )
```

```python
import functools
import math

import jax
import jax.numpy as jnp
from jax import lax
from jax.experimental import pallas as pl
from jax.experimental.pallas import tpu as pltpu
from jax.sharding import PartitionSpec as P

STIFFNESS = 20.0
DAMPING = 0.5
SCALE = math.sqrt(0.5 / math.log(2.0))
LANES = 128
SIDES = 6
BLOCK = SIDES * LANES
F32 = jnp.float32
BF16 = jnp.bfloat16


def split3(x):
    hi = x.astype(BF16).astype(F32)
    rest = x - hi
    mid = rest.astype(BF16).astype(F32)
    return hi, mid, rest - mid


def sin_cos(x):
    k = jnp.floor(x * 0.6366197723675814 + 0.5)
    r = x - k * 1.5703125
    r = r - k * 4.837512969970703125e-4
    r = r - k * 7.54978995489188216e-8
    z = r * r
    s = ((-1.9515295891e-4 * z + 8.3321608736e-3) * z - 1.6666654611e-1) * z * r + r
    c = ((2.443315711809948e-5 * z - 1.388731625493765e-3) * z + 4.166664568298827e-2) * z * z
    c = c - 0.5 * z + 1.0
    q = k.astype(jnp.int32) & 3
    odd = (q & 1) == 1
    sin = jnp.where(odd, c, s)
    cos = jnp.where(odd, s, c)
    sin = jnp.where(q >= 2, -sin, sin)
    cos = jnp.where((q == 1) | (q == 2), -cos, cos)
    return sin, cos


def mm(a, b, contract=((1,), (0,))):
    return lax.dot_general(a, b, (contract, ((), ())), preferred_element_type=F32)


def partner(me, m, n):
    if n & (n - 1):
        return lax.rem(me + m, n)
    to, bit = 0, 1
    while bit < n:
        to = to + bit * lax.rem(me // bit + (m // bit) % 2, 2)
        bit *= 2
    return to


def source_of(me, m, n):
    return lax.rem(me + n - m, n) if n & (n - 1) else partner(me, m, n)


def other(me, u):
    return u + jnp.where(u >= me, 1, 0)


def blocks_of(n, f):
    if n == 1:
        f(0)
    else:
        pl.loop(0, n)(f)


def kernel(
    n_elem, n_buck, node_any, eroded_any, bmap_any, spoint_any, sangle_any, out,
    node, eroded, bmap, perm, spread, pick, rows, faces, wide_faces, onehot, table, values, seg_t, counts,
    sel0, sel1, sel2, sel3, parts,
    in_sem, seg_send, seg_recv, cnt_sem, par_send, par_recv, ready, go,
):
    me = lax.axis_index("elem")
    mb = lax.axis_index("bucket")
    buckets, segs = table.shape[1:]
    own = buckets // n_elem
    count = eroded.shape[1]
    jblocks = count // LANES
    blocks = node.shape[1] // BLOCK
    nfaces = SIDES * count
    chunks, wide = parts.shape[0], parts.shape[3]
    mesh_ids = pl.DeviceIdType.MESH

    barrier = pltpu.get_barrier_semaphore()
    for u in range(n_elem - 1):
        to = {"elem": other(me, u)}
        pl.semaphore_signal(barrier, inc=1, device_id=to, device_id_type=mesh_ids)

    leads = me == 0

    @pl.when(leads)
    def _():
        for d in range(1, n_buck):
            to = {"bucket": lax.rem(mb + d, n_buck)}
            pl.semaphore_signal(barrier, inc=1, device_id=to, device_id_type=mesh_ids)

    def held(owner):
        return table.at[:, pl.ds(pl.multiple_of(owner * own, own), own)]

    mine = pl.ds(pl.multiple_of(me * own, own), own)
    loads = [
        pltpu.make_async_copy(src, dst, in_sem.at[i])
        for i, src, dst in [
            (0, spoint_any, table.at[0:3, mine]),
            (0, sangle_any.at[:, 0], table.at[3, mine]),
            (0, sangle_any.at[:, 1], table.at[4, mine]),
            (1, eroded_any, eroded),
            (2, bmap_any, bmap),
            (3, node_any, node),
        ]
    ]
    for load in loads:
        load.start()

    col = lax.broadcasted_iota(jnp.int32, (1, BLOCK), 1)
    source = SIDES * (col & (LANES - 1)) + (col // LANES)
    for i in range(BLOCK // 256):
        r = lax.broadcasted_iota(jnp.int32, (256, BLOCK), 0) + i * 256
        perm[i * 256:(i + 1) * 256, :] = jnp.where(r == source, 1.0, 0.0).astype(BF16)

    first = SIDES * lax.broadcasted_iota(jnp.int32, (LANES, BLOCK), 0)
    away = lax.broadcasted_iota(jnp.int32, (LANES, BLOCK), 1) - first
    spread[...] = jnp.where((away >= 0) & (away < SIDES), 1.0, 0.0).astype(BF16)

    def seg_copy(owner, target):
        return pltpu.make_async_remote_copy(
            src_ref=held(owner), dst_ref=held(owner),
            send_sem=seg_send, recv_sem=seg_recv.at[owner - jnp.where(owner > target, 1, 0)],
            device_id={"elem": target}, device_id_type=mesh_ids,
        )

    chunk = min(buckets, LANES)

    def tally():
        loads[3].wait()
        loads[4].wait()
        erode = eroded[...]
        high = lax.broadcasted_iota(jnp.int32, (blocks, count), 0) == erode // LANES
        low = lax.broadcasted_iota(jnp.int32, (LANES, count), 0) == lax.rem(erode, LANES)
        mask = mm(
            jnp.where(high, 1.0, 0.0).astype(BF16), jnp.where(low, 1.0, 0.0).astype(BF16), ((1,), (1,))
        )
        mask = mm(mask.astype(BF16), spread[...])

        def count_block(b):
            iota = lax.broadcasted_iota(jnp.int32, (chunk, LANES), 0) + b * chunk
            total = jnp.zeros((chunk, LANES), F32)
            for r in range(blocks):
                ids = jnp.where(mask[r:r + 1] > 0.5, bmap[:, r * BLOCK:(r + 1) * BLOCK], -1)
                for g in range(SIDES):
                    hit = iota == ids[:, g * LANES:(g + 1) * LANES]
                    total = total + jnp.where(hit, 1.0, 0.0)
            if chunk < LANES:
                total = jnp.concatenate([total, jnp.zeros((LANES - chunk, LANES), F32)], axis=0)
            sums = mm(jnp.ones((8, LANES), BF16), total.astype(BF16), ((1,), (1,)))
            at = 0 if buckets <= LANES else pl.ds(pl.multiple_of(b * LANES, LANES), LANES)
            if buckets <= LANES:
                counts[me] = sums[0:1]
            else:
                counts[me, :, at] = sums[0:1]

        blocks_of(buckets // chunk, count_block)

    def gather():
        for i in range(pick.shape[0] // 256):
            r = lax.broadcasted_iota(jnp.int32, (256, count), 0) + i * 256
            pick[i * 256:(i + 1) * 256, :] = jnp.where(r == eroded[...], 1.0, 0.0).astype(BF16)

        loads[5].wait()
        group = 4
        for g in range(blocks // group):
            stack = []
            for i in range(g * group, (g + 1) * group):
                lanes = slice(i * BLOCK, (i + 1) * BLOCK)
                c = [node[3 * v:3 * v + 3, lanes] for v in range(8)]
                e1, e2 = c[2] - c[0], c[3] - c[1]
                r1 = jnp.concatenate([e1[1:3], e1[0:1]], axis=0)
                r2 = jnp.concatenate([e2[1:3], e2[0:1]], axis=0)
                area = 0.5 * (e1 * r2 - r1 * e2)
                centroid = 0.25 * (((c[0] + c[1]) + c[2]) + c[3])
                velocity = 0.25 * (((c[4] + c[5]) + c[6]) + c[7])
                ids = bmap[:, lanes].astype(F32)
                two = jnp.zeros((2, BLOCK), F32)
                four = jnp.zeros((4, BLOCK), F32)
                first = jnp.concatenate([centroid, area, two], axis=0)
                second = jnp.concatenate([velocity, ids, four], axis=0)
                a, b = split3(first), split3(second)
                stack += [a[0], b[0], a[1], b[1], a[2]]
            apart = mm(jnp.concatenate(stack, axis=0).astype(BF16), perm[...]).astype(BF16)
            for i in range(group):
                at = (g * group + i) * LANES
                for s in range(SIDES):
                    rows[s * 40:(s + 1) * 40, at:at + LANES] = apart[
                        i * 40:(i + 1) * 40, s * LANES:(s + 1) * LANES
                    ]

        taken = mm(rows[...], pick[...]).astype(BF16)
        stack = []
        for j in range(jblocks):
            lanes = slice(j * LANES, (j + 1) * LANES)
            stack.append(
                jnp.concatenate([taken[s * 40:(s + 1) * 40, lanes] for s in range(SIDES)], axis=1)
            )
        mixed = mm(jnp.concatenate(stack, axis=0), perm[...], ((1,), (1,)))
        for j in range(jblocks):
            t = [mixed[j * 40 + i * 8:j * 40 + i * 8 + 8] for i in range(5)]
            lanes = slice(j * BLOCK, (j + 1) * BLOCK)
            first = (t[0] + t[2]) + t[4]
            second = t[1] + t[3]
            faces[:, lanes] = second[3:4]
            first = jnp.concatenate([SCALE * first[0:3], first[3:8]], axis=0)
            second = (DAMPING / SCALE) * second
            for i in range(SIDES):
                cut = slice(i * LANES, (i + 1) * LANES)
                for q in range(9):
                    row = first[q:q + 1, cut] if q < 6 else second[q - 6:q - 5, cut]
                    wide_faces[j * SIDES + i, q * 8:q * 8 + 8, :] = jnp.broadcast_to(row, (8, LANES))

        def hot_block(b):
            for j in range(nfaces // 512):
                lanes = slice(j * 512, (j + 1) * 512)
                iota = lax.broadcasted_iota(jnp.int32, (chunk, 512), 0) + b * chunk
                hit = iota == faces[:, lanes].astype(jnp.int32)
                onehot[pl.ds(b * chunk, chunk), lanes] = jnp.where(hit, 1.0, 0.0).astype(BF16)

        blocks_of(buckets // chunk, hot_block)

    @pl.when(leads)
    def _():
        tally()
        gather()

    pltpu.make_async_copy(held(me), held(me), in_sem.at[0]).wait()
    pl.semaphore_wait(barrier, n_elem - 1 + jnp.where(leads, n_buck - 1, 0))

    seg_copy(me, other(me, 0)).start()

    @pl.when(leads)
    def _():
        for d in range(1, n_buck):
            to = {"bucket": lax.rem(mb + d, n_buck)}
            pl.semaphore_signal(ready, inc=1, device_id=to, device_id_type=mesh_ids)

    def cnt_copy(at, target):
        return pltpu.make_async_remote_copy(
            src_ref=counts.at[at], dst_ref=counts.at[at],
            send_sem=cnt_sem.at[0], recv_sem=cnt_sem.at[1],
            device_id={"elem": target}, device_id_type=mesh_ids,
        )

    @pl.when(jnp.logical_not(leads))
    def _():
        tally()

    for u in range(n_elem - 1):
        cnt_copy(me, other(me, u)).start()
    for u in range(1, n_elem - 1):
        seg_copy(me, other(me, u)).start()

    @pl.when(jnp.logical_not(leads))
    def _():
        gather()

    @pl.when(leads)
    def _():
        pl.semaphore_wait(ready, n_buck - 1)
        for u in range(n_elem - 1):
            to = {"elem": other(me, u)}
            pl.semaphore_signal(go, inc=1, device_id=to, device_id_type=mesh_ids)

    def unfold(owner):
        at = pl.ds(pl.multiple_of(owner * own, own), own)
        sin0, cos0 = sin_cos(table[3, at, :])
        sin1, cos1 = sin_cos(table[4, at, :])
        x, y, z = [SCALE * table[i, at, :] for i in range(3)]
        for i, v in enumerate([x, y, z, cos0 * sin1, sin0 * sin1, cos1]):
            values[i, at, :] = v

    unfold(me)
    for m in range(1, n_elem):
        owner = source_of(me, m, n_elem)
        seg_copy(owner, me).wait_recv()
        unfold(owner)
    cnt_copy(pl.ds(0, n_elem - 1), me).wait_recv()

    chunk = min(buckets, LANES // 2)

    def lay_out(b):
        for i in range(6):
            v = values[i, pl.ds(pl.multiple_of(b * chunk, chunk), chunk), :]
            stack = jnp.concatenate(list(split3(v)) + [jnp.zeros_like(v)], axis=0).astype(BF16)
            for h in range(4 * chunk // LANES):
                lanes = pl.ds(pl.multiple_of(b * 4 * chunk + h * LANES, LANES), LANES)
                seg_t[i * segs:(i + 1) * segs, lanes] = stack[h * LANES:(h + 1) * LANES].T

    blocks_of(buckets // chunk, lay_out)

    whole = counts[0]
    for i in range(1, n_elem):
        whole = whole + counts[i]
    stiff = (STIFFNESS / SCALE) * lax.rsqrt(jnp.maximum(whole[:, :buckets], 1.0))
    hi, mid, lo = split3(jnp.broadcast_to(stiff, (16, buckets)))
    pieces = []
    for b in range(0, buckets, chunk):
        cut = slice(b, b + chunk)
        pieces += [hi[:, cut], mid[:, cut], lo[:, cut], jnp.zeros((16, chunk), F32)]
    seg_t[6 * segs:6 * segs + 16, :] = jnp.concatenate(pieces, axis=1).astype(BF16)

    half = 256
    steps = nfaces // half

    def select(it, sel):
        hot = onehot[:, pl.ds(pl.multiple_of(it * half, half), half)]
        hot = [hot[b:b + chunk] for b in range(0, buckets, chunk) for _ in range(4)]
        sel[...] = mm(seg_t[...], jnp.concatenate(hot, axis=0))

    def forces(it, c, at, sel):
        for lt in range(half // LANES):
            row = it * (half // LANES) + lt
            cx, cy, cz, az, ax, ay, vx, vy, vz = [
                wide_faces[row, q * 8:q * 8 + 8, :] for q in range(9)
            ]
            tile = slice(lt * LANES, (lt + 1) * LANES)
            stf = sel[6 * segs:6 * segs + 8, tile]
            acc = [jnp.zeros((8, LANES), F32) for _ in range(3)]
            for r in range(segs // 8):
                px, py, pz, nx, ny, nz = [
                    sel[q * segs + r * 8:q * segs + r * 8 + 8, tile] for q in range(6)
                ]
                ox, oy, oz = px - cx, py - cy, pz - cz
                dist = ox * ox + oy * oy + oz * oz
                depth = jnp.maximum(ox * nx + oy * ny + oz * nz, 0.0)
                proj = jnp.abs(ax * nx + ay * ny + az * nz)
                push = stf - (vx * nx + vy * ny + vz * nz)
                traction = (jnp.exp2(-dist) * depth) * (push * proj)
                for k, n in enumerate((nx, ny, nz)):
                    acc[k] = acc[k] + traction * n
            for k in range(3):
                total = jnp.sum(acc[k], axis=0, keepdims=True)
                parts[c, mb, k:k + 1, at + lt * LANES:at + (lt + 1) * LANES] = total

    def par_copy(at, who, some, target):
        return pltpu.make_async_remote_copy(
            src_ref=parts.at[at, who], dst_ref=parts.at[at, who],
            send_sem=par_send, recv_sem=par_recv.at[some],
            device_id={"bucket": target}, device_id_type=mesh_ids,
        )

    targets = [partner(mb, m, n_buck) for m in sorted(range(1, n_buck), key=lambda m: m == 1)]
    pair = [(sel0, sel1), (sel2, sel3)]
    select(0, sel0)
    select(1, sel1)

    def block(c, now, later):
        it = 2 * c
        for i in range(2):
            ahead = it + 2 + i
            select(jnp.where(ahead < steps, ahead, i), later[i])
        for i in range(2):
            forces(it + i, c, i * half, now[i])
        last = jnp.where(c == chunks - 1, 1, 0)
        for target in targets:
            par_copy(c, mb, last, target).start()

    def step(i, carry):
        once = jnp.minimum(me + 1, 1)
        pl.loop(0, once)(lambda _: block(2 * i, pair[0], pair[1]))
        pl.loop(0, once)(lambda _: block(2 * i + 1, pair[1], pair[0]))
        return carry

    @pl.when(jnp.logical_not(leads))
    def _():
        pl.semaphore_wait(go, 1)

    lax.fori_loop(0, chunks // 2, step, 0)

    others = pl.ds(0, n_buck - 1)

    def finish(c):
        force = parts[c, 0]
        for i in range(1, n_buck):
            force = force + parts[c, i]
        out[:, c * wide:(c + 1) * wide] = force

    par_copy(pl.ds(0, chunks - 1), others, 0, mb).wait_recv()
    for c in range(chunks - 1):
        finish(c)
    par_copy(pl.ds(chunks - 1, 1), others, 1, mb).wait_recv()
    finish(chunks - 1)

    rest = pl.ds(0, own * (n_elem - 1))
    pltpu.make_async_copy(table.at[:, rest], table.at[:, rest], seg_send).wait()
    cnt_copy(pl.ds(0, n_elem - 1), me).wait_send()
    par_copy(pl.ds(0, chunks), others, 0, mb).wait_send()


def local(n_elem, n_buck, node_data, eroded, bucket_map, seg_point, seg_angle):
    own, _, segs = seg_point.shape
    buckets = own * n_elem
    count = eroded.shape[0]
    elems = node_data.shape[1] // SIDES
    nfaces = SIDES * count
    wide = 512
    dma = pltpu.SemaphoreType.DMA
    points = seg_point.transpose(1, 0, 2)
    operands = (node_data, eroded[None, :], bucket_map[None, :], points, seg_angle)
    scratch = [
        (node_data.shape, F32),
        ((1, count), jnp.int32),
        ((1, node_data.shape[1]), jnp.int32),
        ((BLOCK, BLOCK), BF16),
        ((LANES, BLOCK), BF16),
        ((elems, count), BF16),
        ((SIDES * 40, elems), BF16),
        ((1, nfaces), F32),
        ((nfaces // LANES, 72, LANES), F32),
        ((buckets, nfaces), BF16),
        ((5, buckets, segs), F32),
        ((6, buckets, segs), F32),
        ((6 * segs + 16, 4 * buckets), BF16),
        ((n_elem, 1, max(buckets, LANES)), F32),
        ((6 * segs + 16, 256), F32),
        ((6 * segs + 16, 256), F32),
        ((6 * segs + 16, 256), F32),
        ((6 * segs + 16, 256), F32),
        ((nfaces // wide, n_buck, 3, wide), F32),
    ]
    need = sum(math.prod(shape) * jnp.dtype(kind).itemsize for shape, kind in scratch)
    return pl.pallas_call(
        functools.partial(kernel, n_elem, n_buck),
        out_shape=jax.ShapeDtypeStruct((3, nfaces), F32),
        in_specs=[pl.BlockSpec(memory_space=pltpu.HBM)] * 5,
        out_specs=pl.BlockSpec(memory_space=pltpu.VMEM),
        scratch_shapes=[pltpu.VMEM(shape, kind) for shape, kind in scratch]
        + [
            dma((4,)),
            dma,
            dma((n_elem - 1,)),
            dma((2,)),
            dma,
            dma((2,)),
            pltpu.SemaphoreType.REGULAR,
            pltpu.SemaphoreType.REGULAR,
        ],
        compiler_params=pltpu.CompilerParams(
            collective_id=0, has_side_effects=True,
            vmem_limit_bytes=need + 12 * 1024 * 1024,
        ),
        name="contact",
    )(*[pltpu.with_memory_space_constraint(x, pltpu.HBM) for x in operands])


def solution(mesh):
    in_specs = (
        P(None, "elem"),
        P("elem"),
        P("elem"),
        P("elem", None, "bucket"),
        P("elem", None, "bucket"),
    )
    body = functools.partial(local, mesh.shape["elem"], mesh.shape["bucket"])
    return jax.shard_map(
        body, mesh=mesh, in_specs=in_specs, out_specs=P(None, "elem"), check_vma=False
    )
```

```python
import functools
import math

import jax
import jax.numpy as jnp
from jax import lax
from jax.experimental import pallas as pl
from jax.experimental.pallas import tpu as pltpu
from jax.sharding import PartitionSpec as P

STIFFNESS = 20.0
DAMPING = 0.5
SCALE = math.sqrt(0.5 / math.log(2.0))
LANES = 128
SIDES = 6
BLOCK = SIDES * LANES
F32 = jnp.float32
BF16 = jnp.bfloat16


def split3(x):
    hi = x.astype(BF16).astype(F32)
    rest = x - hi
    mid = rest.astype(BF16).astype(F32)
    return hi, mid, rest - mid


def sin_cos(x):
    k = jnp.floor(x * 0.6366197723675814 + 0.5)
    r = x - k * 1.5703125
    r = r - k * 4.837512969970703125e-4
    r = r - k * 7.54978995489188216e-8
    z = r * r
    s = ((-1.9515295891e-4 * z + 8.3321608736e-3) * z - 1.6666654611e-1) * z * r + r
    c = ((2.443315711809948e-5 * z - 1.388731625493765e-3) * z + 4.166664568298827e-2) * z * z
    c = c - 0.5 * z + 1.0
    q = k.astype(jnp.int32) & 3
    odd = (q & 1) == 1
    sin = jnp.where(odd, c, s)
    cos = jnp.where(odd, s, c)
    sin = jnp.where(q >= 2, -sin, sin)
    cos = jnp.where((q == 1) | (q == 2), -cos, cos)
    return sin, cos


def mm(a, b, contract=((1,), (0,))):
    return lax.dot_general(a, b, (contract, ((), ())), preferred_element_type=F32)


def partner(me, m, n):
    if n & (n - 1):
        return lax.rem(me + m, n)
    to, bit = 0, 1
    while bit < n:
        to = to + bit * lax.rem(me // bit + (m // bit) % 2, 2)
        bit *= 2
    return to


def source_of(me, m, n):
    return lax.rem(me + n - m, n) if n & (n - 1) else partner(me, m, n)


def other(me, u):
    return u + jnp.where(u >= me, 1, 0)


def blocks_of(n, f):
    if n == 1:
        f(0)
    else:
        pl.loop(0, n)(f)


def kernel(
    n_elem, n_buck, node_any, eroded_any, bmap_any, spoint_any, sangle_any, out,
    node, eroded, bmap, perm, pick, rows, faces, wide_faces, onehot, table, values, seg_t, counts,
    sel0, sel1, sel2, sel3, parts,
    in_sem, seg_send, seg_recv, cnt_sem, par_send, par_recv, up, ready, go,
):
    me = lax.axis_index("elem")
    mb = lax.axis_index("bucket")
    buckets, segs = table.shape[1:]
    own = buckets // n_elem
    count = eroded.shape[1]
    jblocks = count // LANES
    blocks = node.shape[1] // BLOCK
    nfaces = SIDES * count
    chunks, wide = parts.shape[0], parts.shape[3]
    mesh_ids = pl.DeviceIdType.MESH

    barrier = pltpu.get_barrier_semaphore()
    for t in range(1, n_elem):
        @pl.when(me < t)
        def _():
            pl.semaphore_signal(barrier, inc=1, device_id={"elem": t}, device_id_type=mesh_ids)

    leads = me == 0

    @pl.when(leads)
    def _():
        for d in range(1, n_buck):
            to = {"bucket": lax.rem(mb + d, n_buck)}
            pl.semaphore_signal(barrier, inc=1, device_id=to, device_id_type=mesh_ids)

    def held(owner):
        return table.at[:, pl.ds(pl.multiple_of(owner * own, own), own)]

    mine = pl.ds(pl.multiple_of(me * own, own), own)
    loads = [
        pltpu.make_async_copy(src, dst, in_sem.at[i])
        for i, src, dst in [
            (1, eroded_any, eroded),
            (0, spoint_any, table.at[0:3, mine]),
            (0, sangle_any.at[:, 0], table.at[3, mine]),
            (0, sangle_any.at[:, 1], table.at[4, mine]),
            (2, bmap_any, bmap),
            (3, node_any, node),
        ]
    ]
    for load in loads:
        load.start()

    col = lax.broadcasted_iota(jnp.int32, (1, BLOCK), 1)
    source = SIDES * (col & (LANES - 1)) + (col // LANES)
    for i in range(BLOCK // 256):
        r = lax.broadcasted_iota(jnp.int32, (256, BLOCK), 0) + i * 256
        perm[i * 256:(i + 1) * 256, :] = jnp.where(r == source, 1.0, 0.0).astype(BF16)

    def seg_copy(owner, target):
        return pltpu.make_async_remote_copy(
            src_ref=held(owner), dst_ref=held(owner),
            send_sem=seg_send, recv_sem=seg_recv.at[owner - jnp.where(owner > target, 1, 0)],
            device_id={"elem": target}, device_id_type=mesh_ids,
        )

    chunk = min(buckets, LANES)

    def tally():
        loads[0].wait()
        loads[4].wait()
        erode = eroded[...]
        high = lax.broadcasted_iota(jnp.int32, (blocks, count), 0) == erode // LANES
        low = lax.broadcasted_iota(jnp.int32, (LANES, count), 0) == lax.rem(erode, LANES)
        mask = mm(
            jnp.where(high, 1.0, 0.0).astype(BF16), jnp.where(low, 1.0, 0.0).astype(BF16), ((1,), (1,))
        )
        lane = lax.broadcasted_iota(jnp.int32, (blocks, LANES), 1)
        picked = [
            jnp.take_along_axis(mask, (lane + g * LANES) // SIDES, axis=1) for g in range(SIDES)
        ]

        def count_block(b):
            iota = lax.broadcasted_iota(jnp.int32, (chunk, LANES), 0) + b * chunk
            total = jnp.zeros((chunk, LANES), F32)
            for r in range(blocks):
                for g in range(SIDES):
                    at = r * BLOCK + g * LANES
                    ids = jnp.where(picked[g][r:r + 1] > 0.5, bmap[:, at:at + LANES], -1)
                    hit = iota == ids
                    total = total + jnp.where(hit, 1.0, 0.0)
            if chunk < LANES:
                total = jnp.concatenate([total, jnp.zeros((LANES - chunk, LANES), F32)], axis=0)
            sums = jnp.sum(total.T, axis=0, keepdims=True)
            at = 0 if buckets <= LANES else pl.ds(pl.multiple_of(b * LANES, LANES), LANES)
            if buckets <= LANES:
                counts[me] = sums
            else:
                counts[me, :, at] = sums

        blocks_of(buckets // chunk, count_block)

    def gather():
        for i in range(pick.shape[0] // 256):
            r = lax.broadcasted_iota(jnp.int32, (256, count), 0) + i * 256
            pick[i * 256:(i + 1) * 256, :] = jnp.where(r == eroded[...], 1.0, 0.0).astype(BF16)

        loads[5].wait()
        group = 4
        for g in range(blocks // group):
            stack = []
            for i in range(g * group, (g + 1) * group):
                lanes = slice(i * BLOCK, (i + 1) * BLOCK)
                c = [node[3 * v:3 * v + 3, lanes] for v in range(8)]
                e1, e2 = c[2] - c[0], c[3] - c[1]
                r1 = jnp.concatenate([e1[1:3], e1[0:1]], axis=0)
                r2 = jnp.concatenate([e2[1:3], e2[0:1]], axis=0)
                area = 0.5 * (e1 * r2 - r1 * e2)
                centroid = 0.25 * (((c[0] + c[1]) + c[2]) + c[3])
                velocity = 0.25 * (((c[4] + c[5]) + c[6]) + c[7])
                ids = bmap[:, lanes].astype(F32)
                two = jnp.zeros((2, BLOCK), F32)
                four = jnp.zeros((4, BLOCK), F32)
                first = jnp.concatenate([centroid, area, two], axis=0)
                second = jnp.concatenate([velocity, ids, four], axis=0)
                a, b = split3(first), split3(second)
                stack += [a[0], b[0], a[1], b[1], a[2]]
            apart = mm(jnp.concatenate(stack, axis=0).astype(BF16), perm[...]).astype(BF16)
            for i in range(group):
                at = (g * group + i) * LANES
                for s in range(SIDES):
                    rows[s * 40:(s + 1) * 40, at:at + LANES] = apart[
                        i * 40:(i + 1) * 40, s * LANES:(s + 1) * LANES
                    ]

        taken = mm(rows[...], pick[...]).astype(BF16)
        stack = []
        for j in range(jblocks):
            lanes = slice(j * LANES, (j + 1) * LANES)
            stack.append(
                jnp.concatenate([taken[s * 40:(s + 1) * 40, lanes] for s in range(SIDES)], axis=1)
            )
        mixed = mm(jnp.concatenate(stack, axis=0), perm[...], ((1,), (1,)))
        for j in range(jblocks):
            t = [mixed[j * 40 + i * 8:j * 40 + i * 8 + 8] for i in range(5)]
            lanes = slice(j * BLOCK, (j + 1) * BLOCK)
            first = (t[0] + t[2]) + t[4]
            second = t[1] + t[3]
            faces[:, lanes] = second[3:4]
            first = jnp.concatenate([SCALE * first[0:3], first[3:8]], axis=0)
            second = (DAMPING / SCALE) * second
            for i in range(SIDES):
                cut = slice(i * LANES, (i + 1) * LANES)
                for q in range(9):
                    row = first[q:q + 1, cut] if q < 6 else second[q - 6:q - 5, cut]
                    wide_faces[j * SIDES + i, q * 8:q * 8 + 8, :] = jnp.broadcast_to(row, (8, LANES))

        def hot_block(b):
            for j in range(nfaces // 512):
                lanes = slice(j * 512, (j + 1) * 512)
                iota = lax.broadcasted_iota(jnp.int32, (chunk, 512), 0) + b * chunk
                hit = iota == faces[:, lanes].astype(jnp.int32)
                onehot[pl.ds(b * chunk, chunk), lanes] = jnp.where(hit, 1.0, 0.0).astype(BF16)

        blocks_of(buckets // chunk, hot_block)

    @pl.when(leads)
    def _():
        tally()
        gather()
        pl.semaphore_wait(barrier, n_buck - 1)

    @pl.when(jnp.logical_not(leads))
    def _():
        pl.semaphore_wait(barrier, me)

    for t in range(n_elem - 1):
        @pl.when(me > t)
        def _():
            pl.semaphore_signal(up, inc=1, device_id={"elem": t}, device_id_type=mesh_ids)

    pltpu.make_async_copy(held(me), held(me), in_sem.at[0]).wait()
    @pl.when(jnp.logical_not(leads))
    def _():
        seg_copy(me, 0).start()

    def cnt_copy(at, target):
        return pltpu.make_async_remote_copy(
            src_ref=counts.at[at], dst_ref=counts.at[at],
            send_sem=cnt_sem.at[0], recv_sem=cnt_sem.at[1],
            device_id={"elem": target}, device_id_type=mesh_ids,
        )

    @pl.when(jnp.logical_not(leads))
    def _():
        tally()

    for t in range(n_elem - 1):
        @pl.when(me > t)
        def _():
            cnt_copy(me, t).start()
    for t in range(1, n_elem - 1):
        @pl.when(me > t)
        def _():
            seg_copy(me, t).start()

    @pl.when(me < n_elem - 1)
    def _():
        pl.semaphore_wait(up, n_elem - 1 - me)

    @pl.when(leads)
    def _():
        for d in range(1, n_buck):
            to = {"bucket": lax.rem(mb + d, n_buck)}
            pl.semaphore_signal(ready, inc=1, device_id=to, device_id_type=mesh_ids)

    for t in range(1, n_elem):
        @pl.when(me < t)
        def _():
            cnt_copy(me, t).start()
            seg_copy(me, t).start()

    @pl.when(jnp.logical_not(leads))
    def _():
        gather()

    @pl.when(leads)
    def _():
        pl.semaphore_wait(ready, n_buck - 1)
        for u in range(n_elem - 1):
            to = {"elem": other(me, u)}
            pl.semaphore_signal(go, inc=1, device_id=to, device_id_type=mesh_ids)

    def unfold(owner):
        at = pl.ds(pl.multiple_of(owner * own, own), own)
        sin0, cos0 = sin_cos(table[3, at, :])
        sin1, cos1 = sin_cos(table[4, at, :])
        x, y, z = [SCALE * table[i, at, :] for i in range(3)]
        for i, v in enumerate([x, y, z, cos0 * sin1, sin0 * sin1, cos1]):
            values[i, at, :] = v

    unfold(me)
    for m in range(1, n_elem):
        owner = source_of(me, m, n_elem)
        seg_copy(owner, me).wait_recv()
        unfold(owner)
    cnt_copy(pl.ds(0, n_elem - 1), me).wait_recv()

    chunk = min(buckets, LANES // 2)

    def lay_out(b):
        for i in range(6):
            v = values[i, pl.ds(pl.multiple_of(b * chunk, chunk), chunk), :]
            stack = jnp.concatenate(list(split3(v)) + [jnp.zeros_like(v)], axis=0).astype(BF16)
            for h in range(4 * chunk // LANES):
                lanes = pl.ds(pl.multiple_of(b * 4 * chunk + h * LANES, LANES), LANES)
                seg_t[i * segs:(i + 1) * segs, lanes] = stack[h * LANES:(h + 1) * LANES].T

    blocks_of(buckets // chunk, lay_out)

    whole = counts[0]
    for i in range(1, n_elem):
        whole = whole + counts[i]
    stiff = (STIFFNESS / SCALE) * lax.rsqrt(jnp.maximum(whole[:, :buckets], 1.0))
    hi, mid, lo = split3(jnp.broadcast_to(stiff, (16, buckets)))
    pieces = []
    for b in range(0, buckets, chunk):
        cut = slice(b, b + chunk)
        pieces += [hi[:, cut], mid[:, cut], lo[:, cut], jnp.zeros((16, chunk), F32)]
    seg_t[6 * segs:6 * segs + 16, :] = jnp.concatenate(pieces, axis=1).astype(BF16)

    half = 256
    steps = nfaces // half

    def select(it, sel):
        hot = onehot[:, pl.ds(pl.multiple_of(it * half, half), half)]
        hot = [hot[b:b + chunk] for b in range(0, buckets, chunk) for _ in range(4)]
        sel[...] = mm(seg_t[...], jnp.concatenate(hot, axis=0))

    def forces(it, c, at, sel):
        for lt in range(half // LANES):
            row = it * (half // LANES) + lt
            cx, cy, cz, az, ax, ay, vx, vy, vz = [
                wide_faces[row, q * 8:q * 8 + 8, :] for q in range(9)
            ]
            tile = slice(lt * LANES, (lt + 1) * LANES)
            stf = sel[6 * segs:6 * segs + 8, tile]
            acc = [jnp.zeros((8, LANES), F32) for _ in range(3)]
            for r in range(segs // 8):
                px, py, pz, nx, ny, nz = [
                    sel[q * segs + r * 8:q * segs + r * 8 + 8, tile] for q in range(6)
                ]
                ox, oy, oz = px - cx, py - cy, pz - cz
                dist = ox * ox + oy * oy + oz * oz
                depth = jnp.maximum(ox * nx + oy * ny + oz * nz, 0.0)
                proj = jnp.abs(ax * nx + ay * ny + az * nz)
                push = stf - (vx * nx + vy * ny + vz * nz)
                traction = (jnp.exp2(-dist) * depth) * (push * proj)
                for k, n in enumerate((nx, ny, nz)):
                    acc[k] = acc[k] + traction * n
            for k in range(3):
                total = jnp.sum(acc[k], axis=0, keepdims=True)
                parts[c, mb, k:k + 1, at + lt * LANES:at + (lt + 1) * LANES] = total

    def par_copy(at, who, some, target):
        return pltpu.make_async_remote_copy(
            src_ref=parts.at[at, who], dst_ref=parts.at[at, who],
            send_sem=par_send, recv_sem=par_recv.at[some],
            device_id={"bucket": target}, device_id_type=mesh_ids,
        )

    targets = [partner(mb, m, n_buck) for m in sorted(range(1, n_buck), key=lambda m: m == 1)]
    pair = [(sel0, sel1), (sel2, sel3)]
    select(0, sel0)
    select(1, sel1)

    def block(c, now, later):
        it = 2 * c
        for i in range(2):
            ahead = it + 2 + i
            select(jnp.where(ahead < steps, ahead, i), later[i])
        for i in range(2):
            forces(it + i, c, i * half, now[i])
        last = jnp.where(c == chunks - 1, 1, 0)
        for target in targets:
            par_copy(c, mb, last, target).start()

    def step(i, carry):
        once = jnp.minimum(me + 1, 1)
        pl.loop(0, once)(lambda _: block(2 * i, pair[0], pair[1]))
        pl.loop(0, once)(lambda _: block(2 * i + 1, pair[1], pair[0]))
        return carry

    @pl.when(jnp.logical_not(leads))
    def _():
        pl.semaphore_wait(go, 1)

    lax.fori_loop(0, chunks // 2, step, 0)

    others = pl.ds(0, n_buck - 1)

    def finish(c):
        force = parts[c, 0]
        for i in range(1, n_buck):
            force = force + parts[c, i]
        out[:, c * wide:(c + 1) * wide] = force

    par_copy(pl.ds(0, chunks - 1), others, 0, mb).wait_recv()
    for c in range(chunks - 1):
        finish(c)
    par_copy(pl.ds(chunks - 1, 1), others, 1, mb).wait_recv()
    finish(chunks - 1)

    rest = pl.ds(0, own * (n_elem - 1))
    pltpu.make_async_copy(table.at[:, rest], table.at[:, rest], seg_send).wait()
    cnt_copy(pl.ds(0, n_elem - 1), me).wait_send()
    par_copy(pl.ds(0, chunks), others, 0, mb).wait_send()


def local(n_elem, n_buck, node_data, eroded, bucket_map, seg_point, seg_angle):
    own, _, segs = seg_point.shape
    buckets = own * n_elem
    count = eroded.shape[0]
    elems = node_data.shape[1] // SIDES
    nfaces = SIDES * count
    wide = 512
    dma = pltpu.SemaphoreType.DMA
    points = seg_point.transpose(1, 0, 2)
    operands = (node_data, eroded[None, :], bucket_map[None, :], points, seg_angle)
    scratch = [
        (node_data.shape, F32),
        ((1, count), jnp.int32),
        ((1, node_data.shape[1]), jnp.int32),
        ((BLOCK, BLOCK), BF16),
        ((elems, count), BF16),
        ((SIDES * 40, elems), BF16),
        ((1, nfaces), F32),
        ((nfaces // LANES, 72, LANES), F32),
        ((buckets, nfaces), BF16),
        ((5, buckets, segs), F32),
        ((6, buckets, segs), F32),
        ((6 * segs + 16, 4 * buckets), BF16),
        ((n_elem, 1, max(buckets, LANES)), F32),
        ((6 * segs + 16, 256), F32),
        ((6 * segs + 16, 256), F32),
        ((6 * segs + 16, 256), F32),
        ((6 * segs + 16, 256), F32),
        ((nfaces // wide, n_buck, 3, wide), F32),
    ]
    need = sum(math.prod(shape) * jnp.dtype(kind).itemsize for shape, kind in scratch)
    return pl.pallas_call(
        functools.partial(kernel, n_elem, n_buck),
        out_shape=jax.ShapeDtypeStruct((3, nfaces), F32),
        in_specs=[pl.BlockSpec(memory_space=pltpu.HBM)] * 5,
        out_specs=pl.BlockSpec(memory_space=pltpu.VMEM),
        scratch_shapes=[pltpu.VMEM(shape, kind) for shape, kind in scratch]
        + [
            dma((4,)),
            dma,
            dma((n_elem - 1,)),
            dma((2,)),
            dma,
            dma((2,)),
            pltpu.SemaphoreType.REGULAR,
            pltpu.SemaphoreType.REGULAR,
            pltpu.SemaphoreType.REGULAR,
        ],
        compiler_params=pltpu.CompilerParams(
            collective_id=0, has_side_effects=True,
            vmem_limit_bytes=need + 12 * 1024 * 1024,
        ),
        name="contact",
    )(*[pltpu.with_memory_space_constraint(x, pltpu.HBM) for x in operands])


def solution(mesh):
    in_specs = (
        P(None, "elem"),
        P("elem"),
        P("elem"),
        P("elem", None, "bucket"),
        P("elem", None, "bucket"),
    )
    body = functools.partial(local, mesh.shape["elem"], mesh.shape["bucket"])
    return jax.shard_map(
        body, mesh=mesh, in_specs=in_specs, out_specs=P(None, "elem"), check_vma=False
    )
```

```python
import functools
import math

import jax
import jax.numpy as jnp
from jax import lax
from jax.experimental import pallas as pl
from jax.experimental.pallas import tpu as pltpu
from jax.sharding import PartitionSpec as P

STIFFNESS = 20.0
DAMPING = 0.5
SCALE = math.sqrt(0.5 / math.log(2.0))
LANES = 128
SIDES = 6
BLOCK = SIDES * LANES
F32 = jnp.float32
BF16 = jnp.bfloat16


def split3(x):
    hi = x.astype(BF16).astype(F32)
    rest = x - hi
    mid = rest.astype(BF16).astype(F32)
    return hi, mid, rest - mid


def sin_cos(x):
    k = jnp.floor(x * 0.6366197723675814 + 0.5)
    r = x - k * 1.5703125
    r = r - k * 4.837512969970703125e-4
    r = r - k * 7.54978995489188216e-8
    z = r * r
    s = ((-1.9515295891e-4 * z + 8.3321608736e-3) * z - 1.6666654611e-1) * z * r + r
    c = ((2.443315711809948e-5 * z - 1.388731625493765e-3) * z + 4.166664568298827e-2) * z * z
    c = c - 0.5 * z + 1.0
    q = k.astype(jnp.int32) & 3
    odd = (q & 1) == 1
    sin = jnp.where(odd, c, s)
    cos = jnp.where(odd, s, c)
    sin = jnp.where(q >= 2, -sin, sin)
    cos = jnp.where((q == 1) | (q == 2), -cos, cos)
    return sin, cos


def mm(a, b, contract=((1,), (0,))):
    return lax.dot_general(a, b, (contract, ((), ())), preferred_element_type=F32)


def partner(me, m, n):
    if n & (n - 1):
        return lax.rem(me + m, n)
    to, bit = 0, 1
    while bit < n:
        to = to + bit * lax.rem(me // bit + (m // bit) % 2, 2)
        bit *= 2
    return to


def source_of(me, m, n):
    return lax.rem(me + n - m, n) if n & (n - 1) else partner(me, m, n)


def other(me, u):
    return u + jnp.where(u >= me, 1, 0)


def ends_first(those):
    those = list(those)
    return [those.pop(-(i % 2)) for i in range(len(those))]


def blocks_of(n, f):
    if n == 1:
        f(0)
    else:
        pl.loop(0, n)(f)


def kernel(
    n_elem, n_buck, node_any, eroded_any, bmap_any, spoint_any, sangle_any, out,
    node, eroded, bmap, word, slot, perm, pick, rows, faces, wide_faces, onehot, table, values, seg_t, counts,
    sel0, sel1, sel2, sel3, parts,
    in_sem, seg_send, seg_recv, cnt_sem, par_send, par_recv, up, ready, go,
):
    me = lax.axis_index("elem")
    mb = lax.axis_index("bucket")
    buckets, segs = table.shape[1:]
    own = buckets // n_elem
    count = eroded.shape[1]
    jblocks = count // LANES
    blocks = node.shape[1] // BLOCK
    nfaces = SIDES * count
    chunks, wide = parts.shape[0], parts.shape[3]
    mesh_ids = pl.DeviceIdType.MESH

    barrier = pltpu.get_barrier_semaphore()
    for t in range(1, n_elem):
        @pl.when(me < t)
        def _():
            pl.semaphore_signal(barrier, inc=1, device_id={"elem": t}, device_id_type=mesh_ids)

    leads = me == 0

    @pl.when(leads)
    def _():
        for d in range(1, n_buck):
            to = {"bucket": lax.rem(mb + d, n_buck)}
            pl.semaphore_signal(barrier, inc=1, device_id=to, device_id_type=mesh_ids)

    def held(owner):
        return table.at[:, pl.ds(pl.multiple_of(owner * own, own), own)]

    mine = pl.ds(pl.multiple_of(me * own, own), own)
    loads = [
        pltpu.make_async_copy(src, dst, in_sem.at[i])
        for i, src, dst in [
            (1, eroded_any, eroded),
            (0, spoint_any, table.at[0:3, mine]),
            (0, sangle_any.at[:, 0], table.at[3, mine]),
            (0, sangle_any.at[:, 1], table.at[4, mine]),
        ]
        + [
            (2, bmap_any.at[:, r * BLOCK:(r + 1) * BLOCK], bmap.at[r:r + 1]) for r in range(blocks)
        ]
        + [(3, node_any, node)]
    ]
    for load in loads:
        load.start()

    col = lax.broadcasted_iota(jnp.int32, (1, BLOCK), 1)
    source = SIDES * (col & (LANES - 1)) + (col // LANES)
    for i in range(BLOCK // 256):
        r = lax.broadcasted_iota(jnp.int32, (256, BLOCK), 0) + i * 256
        perm[i * 256:(i + 1) * 256, :] = jnp.where(r == source, 1.0, 0.0).astype(BF16)

    def seg_copy(owner, target):
        return pltpu.make_async_remote_copy(
            src_ref=held(owner), dst_ref=held(owner),
            send_sem=seg_send, recv_sem=seg_recv.at[owner - jnp.where(owner > target, 1, 0)],
            device_id={"elem": target}, device_id_type=mesh_ids,
        )

    chunk = min(buckets, LANES)
    assert blocks * SIDES < 256 and chunk % 64 == 0

    def tally():
        loads[0].wait()
        pltpu.make_async_copy(bmap, bmap, in_sem.at[2]).wait()
        erode = eroded[...]
        high = lax.broadcasted_iota(jnp.int32, (blocks, count), 0) == erode // LANES
        low = lax.broadcasted_iota(jnp.int32, (LANES, count), 0) == lax.rem(erode, LANES)
        mask = mm(
            jnp.where(high, 1.0, 0.0).astype(BF16), jnp.where(low, 1.0, 0.0).astype(BF16), ((1,), (1,))
        )
        lane = lax.broadcasted_iota(jnp.int32, (blocks, LANES), 1)
        picked = jnp.concatenate(
            [jnp.take_along_axis(mask, (lane + g * LANES) // SIDES, axis=1) for g in range(SIDES)],
            axis=1,
        )

        def count_block(b):
            iota = lax.broadcasted_iota(jnp.int32, (16, LANES), 0)
            total = []
            for part in range(chunk // 64):
                rel = bmap[...] - (b * chunk + part * 64)
                inside = (picked > 0.5) & (rel >= 0) & (rel < 64)
                field = jnp.left_shift(jnp.ones_like(rel), 8 * ((jnp.right_shift(rel, 4)) & 3))
                word[...] = jnp.where(inside, field, 0)
                slot[...] = rel & 15
                sums = jnp.zeros((16, LANES), jnp.int32)
                for r in range(blocks):
                    for g in range(SIDES):
                        cut = slice(g * LANES, (g + 1) * LANES)
                        hit = iota == slot[r:r + 1, cut]
                        sums = sums + jnp.where(hit, word[r:r + 1, cut], 0)
                for k in range(4):
                    total.append((jnp.right_shift(sums, 8 * k) & 255).astype(F32))
            total = jnp.concatenate(total, axis=0)
            if chunk < LANES:
                total = jnp.concatenate([total, jnp.zeros((LANES - chunk, LANES), F32)], axis=0)
            sums = jnp.sum(total.T, axis=0, keepdims=True)
            at = 0 if buckets <= LANES else pl.ds(pl.multiple_of(b * LANES, LANES), LANES)
            if buckets <= LANES:
                counts[me] = sums
            else:
                counts[me, :, at] = sums

        blocks_of(buckets // chunk, count_block)

    def gather():
        for i in range(pick.shape[0] // 256):
            r = lax.broadcasted_iota(jnp.int32, (256, count), 0) + i * 256
            pick[i * 256:(i + 1) * 256, :] = jnp.where(r == eroded[...], 1.0, 0.0).astype(BF16)

        loads[-1].wait()
        group = 4
        for g in range(blocks // group):
            stack = []
            for i in range(g * group, (g + 1) * group):
                lanes = slice(i * BLOCK, (i + 1) * BLOCK)
                c = [node[3 * v:3 * v + 3, lanes] for v in range(8)]
                e1, e2 = c[2] - c[0], c[3] - c[1]
                r1 = jnp.concatenate([e1[1:3], e1[0:1]], axis=0)
                r2 = jnp.concatenate([e2[1:3], e2[0:1]], axis=0)
                area = 0.5 * (e1 * r2 - r1 * e2)
                centroid = 0.25 * (((c[0] + c[1]) + c[2]) + c[3])
                velocity = 0.25 * (((c[4] + c[5]) + c[6]) + c[7])
                ids = bmap[i:i + 1].astype(F32)
                two = jnp.zeros((2, BLOCK), F32)
                four = jnp.zeros((4, BLOCK), F32)
                first = jnp.concatenate([centroid, area, two], axis=0)
                second = jnp.concatenate([velocity, ids, four], axis=0)
                a, b = split3(first), split3(second)
                stack += [a[0], b[0], a[1], b[1], a[2]]
            apart = mm(jnp.concatenate(stack, axis=0).astype(BF16), perm[...]).astype(BF16)
            for i in range(group):
                at = (g * group + i) * LANES
                for s in range(SIDES):
                    rows[s * 40:(s + 1) * 40, at:at + LANES] = apart[
                        i * 40:(i + 1) * 40, s * LANES:(s + 1) * LANES
                    ]

        taken = mm(rows[...], pick[...]).astype(BF16)
        stack = []
        for j in range(jblocks):
            lanes = slice(j * LANES, (j + 1) * LANES)
            stack.append(
                jnp.concatenate([taken[s * 40:(s + 1) * 40, lanes] for s in range(SIDES)], axis=1)
            )
        mixed = mm(jnp.concatenate(stack, axis=0), perm[...], ((1,), (1,)))
        for j in range(jblocks):
            t = [mixed[j * 40 + i * 8:j * 40 + i * 8 + 8] for i in range(5)]
            lanes = slice(j * BLOCK, (j + 1) * BLOCK)
            first = (t[0] + t[2]) + t[4]
            second = t[1] + t[3]
            faces[:, lanes] = second[3:4]
            first = jnp.concatenate([SCALE * first[0:3], first[3:8]], axis=0)
            second = (DAMPING / SCALE) * second
            for i in range(SIDES):
                cut = slice(i * LANES, (i + 1) * LANES)
                for q in range(9):
                    row = first[q:q + 1, cut] if q < 6 else second[q - 6:q - 5, cut]
                    wide_faces[j * SIDES + i, q * 8:q * 8 + 8, :] = jnp.broadcast_to(row, (8, LANES))

        def hot_block(b):
            for j in range(nfaces // 512):
                lanes = slice(j * 512, (j + 1) * 512)
                iota = lax.broadcasted_iota(jnp.int32, (chunk, 512), 0) + b * chunk
                hit = iota == faces[:, lanes].astype(jnp.int32)
                onehot[pl.ds(b * chunk, chunk), lanes] = jnp.where(hit, 1.0, 0.0).astype(BF16)

        blocks_of(buckets // chunk, hot_block)

    @pl.when(leads)
    def _():
        tally()
        gather()
        pl.semaphore_wait(barrier, n_buck - 1)

    @pl.when(jnp.logical_not(leads))
    def _():
        pl.semaphore_wait(barrier, me)

    for t in range(n_elem - 1):
        @pl.when(me > t)
        def _():
            pl.semaphore_signal(up, inc=1, device_id={"elem": t}, device_id_type=mesh_ids)

    pltpu.make_async_copy(held(me), held(me), in_sem.at[0]).wait()
    @pl.when(jnp.logical_not(leads))
    def _():
        seg_copy(me, 0).start()

    def cnt_copy(at, target):
        return pltpu.make_async_remote_copy(
            src_ref=counts.at[at], dst_ref=counts.at[at],
            send_sem=cnt_sem.at[0], recv_sem=cnt_sem.at[1],
            device_id={"elem": target}, device_id_type=mesh_ids,
        )

    @pl.when(jnp.logical_not(leads))
    def _():
        tally()

    for t in range(n_elem - 1):
        @pl.when(me > t)
        def _():
            cnt_copy(me, t).start()
    for t in range(1, n_elem - 1):
        @pl.when(me > t)
        def _():
            seg_copy(me, t).start()

    @pl.when(me < n_elem - 1)
    def _():
        pl.semaphore_wait(up, n_elem - 1 - me)

    @pl.when(leads)
    def _():
        for d in range(1, n_buck):
            to = {"bucket": lax.rem(mb + d, n_buck)}
            pl.semaphore_signal(ready, inc=1, device_id=to, device_id_type=mesh_ids)

    for t in ends_first(range(2, n_elem, 2)) + ends_first(range(1, n_elem, 2)):
        @pl.when(me < t)
        def _():
            cnt_copy(me, t).start()
            seg_copy(me, t).start()

    @pl.when(jnp.logical_not(leads))
    def _():
        gather()

    @pl.when(leads)
    def _():
        pl.semaphore_wait(ready, n_buck - 1)
        for u in range(n_elem - 1):
            to = {"elem": other(me, u)}
            pl.semaphore_signal(go, inc=1, device_id=to, device_id_type=mesh_ids)

    def unfold(owner):
        at = pl.ds(pl.multiple_of(owner * own, own), own)
        sin0, cos0 = sin_cos(table[3, at, :])
        sin1, cos1 = sin_cos(table[4, at, :])
        x, y, z = [SCALE * table[i, at, :] for i in range(3)]
        for i, v in enumerate([x, y, z, cos0 * sin1, sin0 * sin1, cos1]):
            values[i, at, :] = v

    unfold(me)
    for m in range(1, n_elem):
        owner = source_of(me, m, n_elem)
        seg_copy(owner, me).wait_recv()
        unfold(owner)
    cnt_copy(pl.ds(0, n_elem - 1), me).wait_recv()

    chunk = min(buckets, LANES // 2)

    def lay_out(b):
        for i in range(6):
            v = values[i, pl.ds(pl.multiple_of(b * chunk, chunk), chunk), :]
            stack = jnp.concatenate(list(split3(v)) + [jnp.zeros_like(v)], axis=0).astype(BF16)
            for h in range(4 * chunk // LANES):
                lanes = pl.ds(pl.multiple_of(b * 4 * chunk + h * LANES, LANES), LANES)
                seg_t[i * segs:(i + 1) * segs, lanes] = stack[h * LANES:(h + 1) * LANES].T

    blocks_of(buckets // chunk, lay_out)

    whole = counts[0]
    for i in range(1, n_elem):
        whole = whole + counts[i]
    stiff = (STIFFNESS / SCALE) * lax.rsqrt(jnp.maximum(whole[:, :buckets], 1.0))
    hi, mid, lo = split3(jnp.broadcast_to(stiff, (16, buckets)))
    pieces = []
    for b in range(0, buckets, chunk):
        cut = slice(b, b + chunk)
        pieces += [hi[:, cut], mid[:, cut], lo[:, cut], jnp.zeros((16, chunk), F32)]
    seg_t[6 * segs:6 * segs + 16, :] = jnp.concatenate(pieces, axis=1).astype(BF16)

    half = 256
    steps = nfaces // half

    def select(it, sel):
        hot = onehot[:, pl.ds(pl.multiple_of(it * half, half), half)]
        hot = [hot[b:b + chunk] for b in range(0, buckets, chunk) for _ in range(4)]
        sel[...] = mm(seg_t[...], jnp.concatenate(hot, axis=0))

    def forces(it, c, at, sel):
        for lt in range(half // LANES):
            row = it * (half // LANES) + lt
            cx, cy, cz, az, ax, ay, vx, vy, vz = [
                wide_faces[row, q * 8:q * 8 + 8, :] for q in range(9)
            ]
            tile = slice(lt * LANES, (lt + 1) * LANES)
            stf = sel[6 * segs:6 * segs + 8, tile]
            acc = [jnp.zeros((8, LANES), F32) for _ in range(3)]
            for r in range(segs // 8):
                px, py, pz, nx, ny, nz = [
                    sel[q * segs + r * 8:q * segs + r * 8 + 8, tile] for q in range(6)
                ]
                ox, oy, oz = px - cx, py - cy, pz - cz
                dist = ox * ox + oy * oy + oz * oz
                depth = jnp.maximum(ox * nx + oy * ny + oz * nz, 0.0)
                proj = jnp.abs(ax * nx + ay * ny + az * nz)
                push = stf - (vx * nx + vy * ny + vz * nz)
                traction = (jnp.exp2(-dist) * depth) * (push * proj)
                for k, n in enumerate((nx, ny, nz)):
                    acc[k] = acc[k] + traction * n
            for k in range(3):
                total = jnp.sum(acc[k], axis=0, keepdims=True)
                parts[c, mb, k:k + 1, at + lt * LANES:at + (lt + 1) * LANES] = total

    def par_copy(at, who, some, target):
        return pltpu.make_async_remote_copy(
            src_ref=parts.at[at, who], dst_ref=parts.at[at, who],
            send_sem=par_send, recv_sem=par_recv.at[some],
            device_id={"bucket": target}, device_id_type=mesh_ids,
        )

    targets = [partner(mb, m, n_buck) for m in sorted(range(1, n_buck), key=lambda m: m == 1)]
    pair = [(sel0, sel1), (sel2, sel3)]
    select(0, sel0)
    select(1, sel1)

    def block(c, now, later):
        it = 2 * c
        for i in range(2):
            ahead = it + 2 + i
            select(jnp.where(ahead < steps, ahead, i), later[i])
        for i in range(2):
            forces(it + i, c, i * half, now[i])
        last = jnp.where(c == chunks - 1, 1, 0)
        for target in targets:
            par_copy(c, mb, last, target).start()

    def step(i, carry):
        once = jnp.minimum(me + 1, 1)
        pl.loop(0, once)(lambda _: block(2 * i, pair[0], pair[1]))
        pl.loop(0, once)(lambda _: block(2 * i + 1, pair[1], pair[0]))
        return carry

    @pl.when(jnp.logical_not(leads))
    def _():
        pl.semaphore_wait(go, 1)

    lax.fori_loop(0, chunks // 2, step, 0)

    others = pl.ds(0, n_buck - 1)

    def finish(c):
        force = parts[c, 0]
        for i in range(1, n_buck):
            force = force + parts[c, i]
        out[:, c * wide:(c + 1) * wide] = force

    par_copy(pl.ds(0, chunks - 1), others, 0, mb).wait_recv()
    for c in range(chunks - 1):
        finish(c)
    par_copy(pl.ds(chunks - 1, 1), others, 1, mb).wait_recv()
    finish(chunks - 1)

    rest = pl.ds(0, own * (n_elem - 1))
    pltpu.make_async_copy(table.at[:, rest], table.at[:, rest], seg_send).wait()
    cnt_copy(pl.ds(0, n_elem - 1), me).wait_send()
    par_copy(pl.ds(0, chunks), others, 0, mb).wait_send()


def local(n_elem, n_buck, node_data, eroded, bucket_map, seg_point, seg_angle):
    own, _, segs = seg_point.shape
    buckets = own * n_elem
    count = eroded.shape[0]
    elems = node_data.shape[1] // SIDES
    nfaces = SIDES * count
    wide = 512
    dma = pltpu.SemaphoreType.DMA
    points = seg_point.transpose(1, 0, 2)
    operands = (node_data, eroded[None, :], bucket_map[None, :], points, seg_angle)
    scratch = [
        (node_data.shape, F32),
        ((1, count), jnp.int32),
        ((elems // LANES, BLOCK), jnp.int32),
        ((elems // LANES, BLOCK), jnp.int32),
        ((elems // LANES, BLOCK), jnp.int32),
        ((BLOCK, BLOCK), BF16),
        ((elems, count), BF16),
        ((SIDES * 40, elems), BF16),
        ((1, nfaces), F32),
        ((nfaces // LANES, 72, LANES), F32),
        ((buckets, nfaces), BF16),
        ((5, buckets, segs), F32),
        ((6, buckets, segs), F32),
        ((6 * segs + 16, 4 * buckets), BF16),
        ((n_elem, 1, max(buckets, LANES)), F32),
        ((6 * segs + 16, 256), F32),
        ((6 * segs + 16, 256), F32),
        ((6 * segs + 16, 256), F32),
        ((6 * segs + 16, 256), F32),
        ((nfaces // wide, n_buck, 3, wide), F32),
    ]
    need = sum(math.prod(shape) * jnp.dtype(kind).itemsize for shape, kind in scratch)
    return pl.pallas_call(
        functools.partial(kernel, n_elem, n_buck),
        out_shape=jax.ShapeDtypeStruct((3, nfaces), F32),
        in_specs=[pl.BlockSpec(memory_space=pltpu.HBM)] * 5,
        out_specs=pl.BlockSpec(memory_space=pltpu.VMEM),
        scratch_shapes=[pltpu.VMEM(shape, kind) for shape, kind in scratch]
        + [
            dma((4,)),
            dma,
            dma((n_elem - 1,)),
            dma((2,)),
            dma,
            dma((2,)),
            pltpu.SemaphoreType.REGULAR,
            pltpu.SemaphoreType.REGULAR,
            pltpu.SemaphoreType.REGULAR,
        ],
        compiler_params=pltpu.CompilerParams(
            collective_id=0, has_side_effects=True,
            vmem_limit_bytes=need + 12 * 1024 * 1024,
        ),
        name="contact",
    )(*[pltpu.with_memory_space_constraint(x, pltpu.HBM) for x in operands])


def solution(mesh):
    in_specs = (
        P(None, "elem"),
        P("elem"),
        P("elem"),
        P("elem", None, "bucket"),
        P("elem", None, "bucket"),
    )
    body = functools.partial(local, mesh.shape["elem"], mesh.shape["bucket"])
    return jax.shard_map(
        body, mesh=mesh, in_specs=in_specs, out_specs=P(None, "elem"), check_vma=False
    )
```

```python
import functools
import math

import jax
import jax.numpy as jnp
from jax import lax
from jax.experimental import pallas as pl
from jax.experimental.pallas import tpu as pltpu
from jax.sharding import PartitionSpec as P

STIFFNESS = 20.0
DAMPING = 0.5
SCALE = math.sqrt(0.5 / math.log(2.0))
LANES = 128
SIDES = 6
BLOCK = SIDES * LANES
F32 = jnp.float32
BF16 = jnp.bfloat16


def split3(x):
    hi = x.astype(BF16).astype(F32)
    rest = x - hi
    mid = rest.astype(BF16).astype(F32)
    return hi, mid, rest - mid


def sin_cos(x):
    k = jnp.floor(x * 0.6366197723675814 + 0.5)
    r = x - k * 1.5703125
    r = r - k * 4.837512969970703125e-4
    r = r - k * 7.54978995489188216e-8
    z = r * r
    s = ((-1.9515295891e-4 * z + 8.3321608736e-3) * z - 1.6666654611e-1) * z * r + r
    c = ((2.443315711809948e-5 * z - 1.388731625493765e-3) * z + 4.166664568298827e-2) * z * z
    c = c - 0.5 * z + 1.0
    q = k.astype(jnp.int32) & 3
    odd = (q & 1) == 1
    sin = jnp.where(odd, c, s)
    cos = jnp.where(odd, s, c)
    sin = jnp.where(q >= 2, -sin, sin)
    cos = jnp.where((q == 1) | (q == 2), -cos, cos)
    return sin, cos


def mm(a, b, contract=((1,), (0,))):
    return lax.dot_general(a, b, (contract, ((), ())), preferred_element_type=F32)


def partner(me, m, n):
    if n & (n - 1):
        return lax.rem(me + m, n)
    to, bit = 0, 1
    while bit < n:
        to = to + bit * lax.rem(me // bit + (m // bit) % 2, 2)
        bit *= 2
    return to


def source_of(me, m, n):
    return lax.rem(me + n - m, n) if n & (n - 1) else partner(me, m, n)


def other(me, u):
    return u + jnp.where(u >= me, 1, 0)


def ends_first(those):
    those = list(those)
    return [those.pop(-(i % 2)) for i in range(len(those))]


def blocks_of(n, f):
    if n == 1:
        f(0)
    else:
        pl.loop(0, n)(f)


def kernel(
    n_elem, n_buck, node_any, eroded_any, bmap_any, spoint_any, sangle_any, out,
    node, eroded, bmap, word, slot, perm, pick, rows, faces, wide_faces, onehot, table, values, seg_t, counts,
    sel0, sel1, sel2, sel3, parts,
    in_sem, seg_send, seg_recv, cnt_sem, par_send, par_recv, up, ready, go,
):
    me = lax.axis_index("elem")
    mb = lax.axis_index("bucket")
    buckets, segs = table.shape[1:]
    own = buckets // n_elem
    count = eroded.shape[1]
    jblocks = count // LANES
    blocks = node.shape[1] // BLOCK
    nfaces = SIDES * count
    chunks, wide = parts.shape[0], parts.shape[3]
    mesh_ids = pl.DeviceIdType.MESH

    barrier = pltpu.get_barrier_semaphore()
    for t in range(1, n_elem):
        @pl.when(me < t)
        def _():
            pl.semaphore_signal(barrier, inc=1, device_id={"elem": t}, device_id_type=mesh_ids)

    leads = me == 0

    @pl.when(leads)
    def _():
        for d in range(1, n_buck):
            to = {"bucket": lax.rem(mb + d, n_buck)}
            pl.semaphore_signal(barrier, inc=1, device_id=to, device_id_type=mesh_ids)

    def held(owner):
        return table.at[:, pl.ds(pl.multiple_of(owner * own, own), own)]

    mine = pl.ds(pl.multiple_of(me * own, own), own)
    loads = [
        pltpu.make_async_copy(src, dst, in_sem.at[i])
        for i, src, dst in [
            (1, eroded_any, eroded),
            (0, spoint_any, table.at[0:3, mine]),
            (0, sangle_any.at[:, 0], table.at[3, mine]),
            (0, sangle_any.at[:, 1], table.at[4, mine]),
        ]
        + [
            (2, bmap_any.at[:, r * BLOCK:(r + 1) * BLOCK], bmap.at[r:r + 1]) for r in range(blocks)
        ]
        + [(3, node_any, node)]
    ]
    for load in loads:
        load.start()

    col = lax.broadcasted_iota(jnp.int32, (1, BLOCK), 1)
    source = SIDES * (col & (LANES - 1)) + (col // LANES)
    for i in range(BLOCK // 256):
        r = lax.broadcasted_iota(jnp.int32, (256, BLOCK), 0) + i * 256
        perm[i * 256:(i + 1) * 256, :] = jnp.where(r == source, 1.0, 0.0).astype(BF16)

    def seg_copy(owner, target):
        return pltpu.make_async_remote_copy(
            src_ref=held(owner), dst_ref=held(owner),
            send_sem=seg_send, recv_sem=seg_recv.at[owner - jnp.where(owner > target, 1, 0)],
            device_id={"elem": target}, device_id_type=mesh_ids,
        )

    chunk = min(buckets, LANES)
    assert blocks * SIDES < 256 and chunk % 64 == 0

    def tally():
        loads[0].wait()
        pltpu.make_async_copy(bmap, bmap, in_sem.at[2]).wait()
        erode = eroded[...]
        high = lax.broadcasted_iota(jnp.int32, (blocks, count), 0) == erode // LANES
        low = lax.broadcasted_iota(jnp.int32, (LANES, count), 0) == lax.rem(erode, LANES)
        mask = mm(
            jnp.where(high, 1.0, 0.0).astype(BF16), jnp.where(low, 1.0, 0.0).astype(BF16), ((1,), (1,))
        )
        lane = lax.broadcasted_iota(jnp.int32, (blocks, LANES), 1)
        picked = jnp.concatenate(
            [jnp.take_along_axis(mask, (lane + g * LANES) // SIDES, axis=1) for g in range(SIDES)],
            axis=1,
        )

        def count_block(b):
            iota = lax.broadcasted_iota(jnp.int32, (16, LANES), 0)
            total = []
            for part in range(chunk // 64):
                rel = bmap[...] - (b * chunk + part * 64)
                inside = (picked > 0.5) & (rel >= 0) & (rel < 64)
                field = jnp.left_shift(jnp.ones_like(rel), 8 * ((jnp.right_shift(rel, 4)) & 3))
                word[...] = jnp.where(inside, field, 0)
                slot[...] = rel & 15
                sums = jnp.zeros((16, LANES), jnp.int32)
                for r in range(blocks):
                    for g in range(SIDES):
                        cut = slice(g * LANES, (g + 1) * LANES)
                        hit = iota == slot[r:r + 1, cut]
                        sums = sums + jnp.where(hit, word[r:r + 1, cut], 0)
                for k in range(4):
                    total.append((jnp.right_shift(sums, 8 * k) & 255).astype(F32))
            total = jnp.concatenate(total, axis=0)
            if chunk < LANES:
                total = jnp.concatenate([total, jnp.zeros((LANES - chunk, LANES), F32)], axis=0)
            sums = jnp.sum(total.T, axis=0, keepdims=True)
            at = 0 if buckets <= LANES else pl.ds(pl.multiple_of(b * LANES, LANES), LANES)
            if buckets <= LANES:
                counts[me] = sums
            else:
                counts[me, :, at] = sums

        blocks_of(buckets // chunk, count_block)

    def gather():
        for i in range(pick.shape[0] // 256):
            r = lax.broadcasted_iota(jnp.int32, (256, count), 0) + i * 256
            pick[i * 256:(i + 1) * 256, :] = jnp.where(r == eroded[...], 1.0, 0.0).astype(BF16)

        loads[-1].wait()
        group = 4
        for g in range(blocks // group):
            stack = []
            for i in range(g * group, (g + 1) * group):
                lanes = slice(i * BLOCK, (i + 1) * BLOCK)
                c = [node[3 * v:3 * v + 3, lanes] for v in range(8)]
                e1, e2 = c[2] - c[0], c[3] - c[1]
                r1 = jnp.concatenate([e1[1:3], e1[0:1]], axis=0)
                r2 = jnp.concatenate([e2[1:3], e2[0:1]], axis=0)
                area = 0.5 * (e1 * r2 - r1 * e2)
                centroid = 0.25 * (((c[0] + c[1]) + c[2]) + c[3])
                velocity = 0.25 * (((c[4] + c[5]) + c[6]) + c[7])
                ids = bmap[i:i + 1].astype(F32)
                two = jnp.zeros((2, BLOCK), F32)
                four = jnp.zeros((4, BLOCK), F32)
                first = jnp.concatenate([centroid, area, two], axis=0)
                second = jnp.concatenate([velocity, ids, four], axis=0)
                a, b = split3(first), split3(second)
                stack += [a[0], b[0], a[1], b[1], a[2]]
            apart = mm(jnp.concatenate(stack, axis=0).astype(BF16), perm[...]).astype(BF16)
            for i in range(group):
                at = (g * group + i) * LANES
                for s in range(SIDES):
                    rows[s * 40:(s + 1) * 40, at:at + LANES] = apart[
                        i * 40:(i + 1) * 40, s * LANES:(s + 1) * LANES
                    ]

        taken = mm(rows[...], pick[...]).astype(BF16)
        stack = []
        for j in range(jblocks):
            lanes = slice(j * LANES, (j + 1) * LANES)
            stack.append(
                jnp.concatenate([taken[s * 40:(s + 1) * 40, lanes] for s in range(SIDES)], axis=1)
            )
        mixed = mm(jnp.concatenate(stack, axis=0), perm[...], ((1,), (1,)))
        for j in range(jblocks):
            t = [mixed[j * 40 + i * 8:j * 40 + i * 8 + 8] for i in range(5)]
            lanes = slice(j * BLOCK, (j + 1) * BLOCK)
            first = (t[0] + t[2]) + t[4]
            second = t[1] + t[3]
            faces[:, lanes] = second[3:4]
            first = jnp.concatenate([SCALE * first[0:3], first[3:8]], axis=0)
            second = (DAMPING / SCALE) * second
            for i in range(SIDES):
                cut = slice(i * LANES, (i + 1) * LANES)
                for q in range(9):
                    row = first[q:q + 1, cut] if q < 6 else second[q - 6:q - 5, cut]
                    wide_faces[j * SIDES + i, q * 8:q * 8 + 8, :] = jnp.broadcast_to(row, (8, LANES))

        def hot_block(b):
            for j in range(nfaces // 512):
                lanes = slice(j * 512, (j + 1) * 512)
                iota = lax.broadcasted_iota(jnp.int32, (chunk, 512), 0) + b * chunk
                hit = iota == faces[:, lanes].astype(jnp.int32)
                onehot[pl.ds(b * chunk, chunk), lanes] = jnp.where(hit, 1.0, 0.0).astype(BF16)

        blocks_of(buckets // chunk, hot_block)

    @pl.when(leads)
    def _():
        tally()
        gather()
        pl.semaphore_wait(barrier, n_buck - 1)

    @pl.when(jnp.logical_not(leads))
    def _():
        pl.semaphore_wait(barrier, me)

    for t in range(n_elem - 1):
        @pl.when(me > t)
        def _():
            pl.semaphore_signal(up, inc=1, device_id={"elem": t}, device_id_type=mesh_ids)

    pltpu.make_async_copy(held(me), held(me), in_sem.at[0]).wait()
    @pl.when(jnp.logical_not(leads))
    def _():
        seg_copy(me, 0).start()

    def cnt_copy(at, target):
        return pltpu.make_async_remote_copy(
            src_ref=counts.at[at], dst_ref=counts.at[at],
            send_sem=cnt_sem.at[0], recv_sem=cnt_sem.at[1],
            device_id={"elem": target}, device_id_type=mesh_ids,
        )

    @pl.when(jnp.logical_not(leads))
    def _():
        tally()

    for t in range(n_elem - 1):
        @pl.when(me > t)
        def _():
            cnt_copy(me, t).start()
    for t in range(1, n_elem - 1):
        @pl.when(me > t)
        def _():
            seg_copy(me, t).start()

    @pl.when(me < n_elem - 1)
    def _():
        pl.semaphore_wait(up, n_elem - 1 - me)

    @pl.when(leads)
    def _():
        for d in range(1, n_buck):
            to = {"bucket": lax.rem(mb + d, n_buck)}
            pl.semaphore_signal(ready, inc=1, device_id=to, device_id_type=mesh_ids)

    for t in ends_first(range(2, n_elem, 2)) + ends_first(range(1, n_elem, 2)):
        @pl.when(me < t)
        def _():
            cnt_copy(me, t).start()
            seg_copy(me, t).start()

    @pl.when(jnp.logical_not(leads))
    def _():
        gather()

    @pl.when(leads)
    def _():
        pl.semaphore_wait(ready, n_buck - 1)
        for u in range(n_elem - 1):
            to = {"elem": other(me, u)}
            pl.semaphore_signal(go, inc=1, device_id=to, device_id_type=mesh_ids)

    def unfold(owner):
        at = pl.ds(pl.multiple_of(owner * own, own), own)
        sin0, cos0 = sin_cos(table[3, at, :])
        sin1, cos1 = sin_cos(table[4, at, :])
        x, y, z = [SCALE * table[i, at, :] for i in range(3)]
        for i, v in enumerate([x, y, z, cos0 * sin1, sin0 * sin1, cos1]):
            values[i, at, :] = v

    unfold(me)
    for m in range(1, n_elem):
        owner = source_of(me, m, n_elem)
        seg_copy(owner, me).wait_recv()
        unfold(owner)
    cnt_copy(pl.ds(0, n_elem - 1), me).wait_recv()

    chunk = min(buckets, LANES // 2)

    def lay_out(b):
        for i in range(6):
            v = values[i, pl.ds(pl.multiple_of(b * chunk, chunk), chunk), :]
            stack = jnp.concatenate(list(split3(v)) + [jnp.zeros_like(v)], axis=0).astype(BF16)
            for h in range(4 * chunk // LANES):
                lanes = pl.ds(pl.multiple_of(b * 4 * chunk + h * LANES, LANES), LANES)
                seg_t[i * segs:(i + 1) * segs, lanes] = stack[h * LANES:(h + 1) * LANES].T

    blocks_of(buckets // chunk, lay_out)

    whole = counts[0]
    for i in range(1, n_elem):
        whole = whole + counts[i]
    stiff = (STIFFNESS / SCALE) * lax.rsqrt(jnp.maximum(whole[:, :buckets], 1.0))
    hi, mid, lo = split3(jnp.broadcast_to(stiff, (16, buckets)))
    pieces = []
    for b in range(0, buckets, chunk):
        cut = slice(b, b + chunk)
        pieces += [hi[:, cut], mid[:, cut], lo[:, cut], jnp.zeros((16, chunk), F32)]
    seg_t[6 * segs:6 * segs + 16, :] = jnp.concatenate(pieces, axis=1).astype(BF16)

    half = 256
    steps = nfaces // half

    def select(it, sel):
        hot = onehot[:, pl.ds(pl.multiple_of(it * half, half), half)]
        hot = [hot[b:b + chunk] for b in range(0, buckets, chunk) for _ in range(4)]
        sel[...] = mm(seg_t[...], jnp.concatenate(hot, axis=0))

    def forces(it, c, at, sel):
        for lt in range(half // LANES):
            row = it * (half // LANES) + lt
            cx, cy, cz, az, ax, ay, vx, vy, vz = [
                wide_faces[row, q * 8:q * 8 + 8, :] for q in range(9)
            ]
            tile = slice(lt * LANES, (lt + 1) * LANES)
            stf = sel[6 * segs:6 * segs + 8, tile]
            acc = [jnp.zeros((8, LANES), F32) for _ in range(3)]
            for r in range(segs // 8):
                px, py, pz, nx, ny, nz = [
                    sel[q * segs + r * 8:q * segs + r * 8 + 8, tile] for q in range(6)
                ]
                ox, oy, oz = px - cx, py - cy, pz - cz
                dist = ox * ox + oy * oy + oz * oz
                depth = jnp.maximum(ox * nx + oy * ny + oz * nz, 0.0)
                proj = jnp.abs(ax * nx + ay * ny + az * nz)
                push = stf - (vx * nx + vy * ny + vz * nz)
                traction = (jnp.exp2(-dist) * depth) * (push * proj)
                for k, n in enumerate((nx, ny, nz)):
                    acc[k] = acc[k] + traction * n
            for k in range(3):
                total = jnp.sum(acc[k], axis=0, keepdims=True)
                parts[c, mb, k:k + 1, at + lt * LANES:at + (lt + 1) * LANES] = total

    def par_copy(at, who, some, target, cut=slice(None)):
        return pltpu.make_async_remote_copy(
            src_ref=parts.at[at, who, :, cut], dst_ref=parts.at[at, who, :, cut],
            send_sem=par_send, recv_sem=par_recv.at[some],
            device_id={"bucket": target}, device_id_type=mesh_ids,
        )

    targets = [partner(mb, m, n_buck) for m in sorted(range(1, n_buck), key=lambda m: m == 1)]
    pair = [(sel0, sel1), (sel2, sel3)]
    select(0, sel0)
    select(1, sel1)

    def block(c, now, later):
        it = 2 * c
        for i in range(2):
            select(it + 2 + i, later[i])
        for i in range(2):
            forces(it + i, c, i * half, now[i])
        for target in targets:
            par_copy(c, mb, 0, target).start()

    def close(c, now):
        for i in range(2):
            forces(2 * c + i, c, i * half, now[i])
            for target in targets:
                par_copy(c, mb, 1, target, slice(i * half, (i + 1) * half)).start()

    once = jnp.minimum(me + 1, 1)

    def step(i, carry):
        pl.loop(0, once)(lambda _: block(2 * i, pair[0], pair[1]))
        pl.loop(0, once)(lambda _: block(2 * i + 1, pair[1], pair[0]))
        return carry

    @pl.when(jnp.logical_not(leads))
    def _():
        pl.semaphore_wait(go, 1)

    lax.fori_loop(0, (chunks - 1) // 2, step, 0)
    odd = (chunks - 1) % 2
    if odd:
        pl.loop(0, once)(lambda _: block(chunks - 2, pair[0], pair[1]))
    pl.loop(0, once)(lambda _: close(chunks - 1, pair[odd]))

    others = pl.ds(0, n_buck - 1)

    def finish(c):
        force = parts[c, 0]
        for i in range(1, n_buck):
            force = force + parts[c, i]
        out[:, c * wide:(c + 1) * wide] = force

    par_copy(pl.ds(0, chunks - 1), others, 0, mb).wait_recv()
    for c in range(chunks - 1):
        finish(c)
    par_copy(pl.ds(chunks - 1, 1), others, 1, mb).wait_recv()
    finish(chunks - 1)

    rest = pl.ds(0, own * (n_elem - 1))
    pltpu.make_async_copy(table.at[:, rest], table.at[:, rest], seg_send).wait()
    cnt_copy(pl.ds(0, n_elem - 1), me).wait_send()
    par_copy(pl.ds(0, chunks), others, 0, mb).wait_send()


def local(n_elem, n_buck, node_data, eroded, bucket_map, seg_point, seg_angle):
    own, _, segs = seg_point.shape
    buckets = own * n_elem
    count = eroded.shape[0]
    elems = node_data.shape[1] // SIDES
    nfaces = SIDES * count
    wide = 512
    dma = pltpu.SemaphoreType.DMA
    points = seg_point.transpose(1, 0, 2)
    operands = (node_data, eroded[None, :], bucket_map[None, :], points, seg_angle)
    scratch = [
        (node_data.shape, F32),
        ((1, count), jnp.int32),
        ((elems // LANES, BLOCK), jnp.int32),
        ((elems // LANES, BLOCK), jnp.int32),
        ((elems // LANES, BLOCK), jnp.int32),
        ((BLOCK, BLOCK), BF16),
        ((elems, count), BF16),
        ((SIDES * 40, elems), BF16),
        ((1, nfaces), F32),
        ((nfaces // LANES, 72, LANES), F32),
        ((buckets, nfaces), BF16),
        ((5, buckets, segs), F32),
        ((6, buckets, segs), F32),
        ((6 * segs + 16, 4 * buckets), BF16),
        ((n_elem, 1, max(buckets, LANES)), F32),
        ((6 * segs + 16, 256), F32),
        ((6 * segs + 16, 256), F32),
        ((6 * segs + 16, 256), F32),
        ((6 * segs + 16, 256), F32),
        ((nfaces // wide, n_buck, 3, wide), F32),
    ]
    need = sum(math.prod(shape) * jnp.dtype(kind).itemsize for shape, kind in scratch)
    return pl.pallas_call(
        functools.partial(kernel, n_elem, n_buck),
        out_shape=jax.ShapeDtypeStruct((3, nfaces), F32),
        in_specs=[pl.BlockSpec(memory_space=pltpu.HBM)] * 5,
        out_specs=pl.BlockSpec(memory_space=pltpu.VMEM),
        scratch_shapes=[pltpu.VMEM(shape, kind) for shape, kind in scratch]
        + [
            dma((4,)),
            dma,
            dma((n_elem - 1,)),
            dma((2,)),
            dma,
            dma((2,)),
            pltpu.SemaphoreType.REGULAR,
            pltpu.SemaphoreType.REGULAR,
            pltpu.SemaphoreType.REGULAR,
        ],
        compiler_params=pltpu.CompilerParams(
            collective_id=0, has_side_effects=True,
            vmem_limit_bytes=need + 12 * 1024 * 1024,
        ),
        name="contact",
    )(*[pltpu.with_memory_space_constraint(x, pltpu.HBM) for x in operands])


def solution(mesh):
    in_specs = (
        P(None, "elem"),
        P("elem"),
        P("elem"),
        P("elem", None, "bucket"),
        P("elem", None, "bucket"),
    )
    body = functools.partial(local, mesh.shape["elem"], mesh.shape["bucket"])
    return jax.shard_map(
        body, mesh=mesh, in_specs=in_specs, out_specs=P(None, "elem"), check_vma=False
    )
```
